16 devices in a mesh: data: 4 (over z, y), stage: 4 (over x, core).
Axes of the slice: x: 2, y: 2, z: 2, core: 2. Of those that a mesh axis runs over, the one named last changes fastest.
Arguments:
- x: bfloat16 [64, 256, 768], P('data'), parts along dimension 0
- g: bfloat16 [64, 256, 768], P('data'), parts along dimension 0
- w1: bfloat16 [2, 4, 768, 3072], P(None, 'stage')
- w2: bfloat16 [2, 4, 3072, 768], P(None, 'stage')
Outputs:
- output 1: bfloat16 [64, 256, 768], P('data'), parts along dimension 0
- output 2: bfloat16 [64, 256, 768], P('data'), parts along dimension 0
- output 3: float32 [8, 4, 768, 3072], P('data', 'stage'), parts along dimension 0
- output 4: float32 [8, 4, 3072, 768], P('data', 'stage'), parts along dimension 0
There are 4 independent parts. The reference program is written for one: setup_inputs(seed, part) draws one part's arguments, and reference() takes and returns one part's arrays. A program takes and returns all parts, laid end to end along the dimension named above; an argument that names none is the same for every part.
All inputs are finite; a program needn't handle non-finite values.
Results may differ from the reference program's by a relative error of at most 0.02.
Values are sent between devices in bfloat16 or wider.
A program may use at most 1 GiB of HBM per device.

```python
import jax
import jax.numpy as jnp
from jax import lax

M = 16
B = 256
D = 768
F = 3072
V = 2
S = 4


def gelu(z):
    return 0.5 * z * (1.0 + lax.erf(z * 0.7071067811865476))


def gelu_grad(z):
    return 0.5 * (1.0 + lax.erf(z * 0.7071067811865476)) + z * jnp.exp(-0.5 * z * z) * 0.3989422804014327


def setup_inputs(seed: int = 0, part: int = 0) -> dict:
    ks, kp = jax.random.split(jax.random.PRNGKey(seed))
    kx, kg = jax.random.split(jax.random.fold_in(kp, part))
    k1, k2 = jax.random.split(ks)
    nl = V * S
    x = jax.random.normal(kx, (M, B, D), jnp.float32).astype(jnp.bfloat16)
    g = jax.random.normal(kg, (M, B, D), jnp.float32).astype(jnp.bfloat16)
    w1 = (jax.random.normal(k1, (V, S, D, F), jnp.float32) * D ** -0.5).astype(jnp.bfloat16)
    w2 = (jax.random.normal(k2, (V, S, F, D), jnp.float32) * (2.0 / (nl * F) ** 0.5)).astype(jnp.bfloat16)
    return {'x': x, 'g': g, 'w1': w1, 'w2': w2}


def _layer_fwd(h, w1, w2):
    z = jnp.dot(h, w1, preferred_element_type=jnp.float32)
    u = gelu(z).astype(jnp.bfloat16)
    r = jnp.dot(u, w2, preferred_element_type=jnp.float32)
    return (h.astype(jnp.float32) + r).astype(jnp.bfloat16)


def _layer_bwd(h, w1, w2, dy):
    z = jnp.dot(h, w1, preferred_element_type=jnp.float32)
    u = gelu(z).astype(jnp.bfloat16)
    dw2 = jnp.dot(u.T, dy, preferred_element_type=jnp.float32)
    du = jnp.dot(dy, w2.T, preferred_element_type=jnp.float32)
    dz = (du * gelu_grad(z)).astype(jnp.bfloat16)
    dw1 = jnp.dot(h.T, dz, preferred_element_type=jnp.float32)
    dh = (dy.astype(jnp.float32) + jnp.dot(dz, w1.T, preferred_element_type=jnp.float32)).astype(jnp.bfloat16)
    return dh, dw1, dw2


def reference(x, g, w1, w2):
    w1s = w1.reshape(V * S, D, F)
    w2s = w2.reshape(V * S, F, D)

    def one(carry, xg):
        a1, a2 = carry
        xm, gm = xg

        def fwd(h, w):
            return _layer_fwd(h, w[0], w[1]), h

        y, hs = lax.scan(fwd, xm, (w1s, w2s))

        def bwd(dy, t):
            dh, d1, d2 = _layer_bwd(t[0], t[1], t[2], dy)
            return dh, (d1, d2)

        dx, (d1s, d2s) = lax.scan(bwd, gm, (hs, w1s, w2s), reverse=True)
        return (a1 + d1s, a2 + d2s), (y, dx)

    init = (jnp.zeros((V * S, D, F), jnp.float32), jnp.zeros((V * S, F, D), jnp.float32))
    (a1, a2), (y, dx) = lax.scan(one, init, (x, g))
    return y, dx, a1.reshape(V, S, D, F), a2.reshape(V, S, F, D)
```

```python
import functools

import jax
import jax.numpy as jnp
from jax import lax
from jax.experimental import pallas as pl
from jax.experimental.pallas import tpu as pltpu
from jax.sharding import PartitionSpec as P

BF = jnp.bfloat16
F32 = jnp.float32
MESH = pl.DeviceIdType.MESH
NT = (((1,), (1,)), ((), ()))
GROUP = 8
LEAD = 9
STEP = 3


def _gelu(z):
    return 0.5 * z * (1.0 + lax.erf(z * 0.7071067811865476))


def _gelu_pair(z):
    half = 0.5 * (1.0 + lax.erf(z * 0.7071067811865476))
    return z * half, half + z * jnp.exp(-0.5 * z * z) * 0.3989422804014327


def _dot(a, b):
    return jnp.dot(a, b, preferred_element_type=F32)


def _dot_nt(a, b):
    return lax.dot_general(a, b, NT, preferred_element_type=F32)


def _pipeline(S, V, M, G, x, g, w1_hbm, w2_hbm, u_out, dz_out, h_out, dy_out, r_out,
              w1, w2, hbuf, dybuf, us, ub, dzb, fo, bo,
              f_recv, b_recv, f_send, b_send, h_sem, dy_sem, u_sem, dz_sem, w_sem):
    p = lax.axis_index('stage')
    nxt = lax.rem(p + 1, S)
    prv = lax.rem(p + S - 1, S)
    first = p == 0
    last = p == S - 1
    n = V * M
    F = w1.shape[-1]
    chunk = 256 if F % 256 == 0 else F

    barrier = pltpu.get_barrier_semaphore()
    for q in (prv, nxt):
        pl.semaphore_signal(barrier, inc=1, device_id={'stage': q}, device_id_type=MESH)

    def load_w(v):
        pltpu.make_async_copy(w1_hbm.at[v], w1.at[v], w_sem.at[2 * v]).start()
        pltpu.make_async_copy(w2_hbm.at[v], w2.at[v], w_sem.at[2 * v + 1]).start()

    def wait_w(v):
        pltpu.make_async_copy(w1_hbm.at[v], w1.at[v], w_sem.at[2 * v]).wait()
        pltpu.make_async_copy(w2_hbm.at[v], w2.at[v], w_sem.at[2 * v + 1]).wait()

    def load_x(m):
        pltpu.make_async_copy(x.at[m], hbuf.at[m], f_recv.at[m]).start()

    def load_g(m):
        s = (V - 1) * M + m
        pltpu.make_async_copy(g.at[m], dybuf.at[s], b_recv.at[s]).start()

    @pl.when(first)
    def _():
        load_x(0)

    load_w(0)

    @pl.when(first)
    def _():
        lax.fori_loop(1, M, lambda m, c: (load_x(m), c)[1], 0)

    for v in range(1, V):
        load_w(v)

    @pl.when(last)
    def _():
        lax.fori_loop(0, M, lambda m, c: (load_g(m), c)[1], 0)

    pl.semaphore_wait(barrier, 2)
    wait_w(0)

    def place(i):
        blk, r = i // (V * G), lax.rem(i, V * G)
        return r // G, blk * G + lax.rem(r, G)

    def wait_f_send(s):
        pltpu.make_async_copy(fo.at[s], r_out.at[0], f_send.at[s]).wait()

    def wait_b_send(s):
        pltpu.make_async_copy(bo.at[s], r_out.at[0], b_send.at[s]).wait()

    def wait_uz(s):
        pltpu.make_async_copy(ub.at[s], u_out.at[0], u_sem.at[s]).wait()
        pltpu.make_async_copy(dzb.at[s], dz_out.at[0], dz_sem.at[s]).wait()

    def forward(i):
        v, m = place(i)
        slot = v * M + m
        s = lax.rem(i, 2)
        for vv in range(1, V):
            @pl.when(i == vv * G)
            def _():
                wait_w(vv)
        pltpu.make_async_copy(fo.at[0], hbuf.at[slot], f_recv.at[slot]).wait()
        pltpu.make_async_copy(hbuf.at[slot], h_out.at[slot], h_sem.at[slot]).start()

        @pl.when(i >= 2)
        def _():
            wait_f_send(s)

        for c in range(F // chunk):
            cs = slice(c * chunk, (c + 1) * chunk)
            us[:, cs] = _gelu(_dot(hbuf[slot], w1[v, :, cs])).astype(BF)
        fo[s] = (hbuf[slot].astype(F32) + _dot(us[...], w2[v])).astype(BF)

        final = last & (v == V - 1)

        @pl.when(final)
        def _():
            pltpu.make_async_copy(fo.at[s], r_out.at[m], f_send.at[s]).start()

        @pl.when(jnp.logical_not(final))
        def _():
            to = slot + jnp.where(last, M, 0)
            pltpu.make_async_remote_copy(
                src_ref=fo.at[s], dst_ref=hbuf.at[to], send_sem=f_send.at[s], recv_sem=f_recv.at[to],
                device_id={'stage': nxt}, device_id_type=MESH).start()

    def backward(j):
        vr, m = place(j)
        v = V - 1 - vr
        slot = v * M + m
        s = lax.rem(j, 2)
        pltpu.make_async_copy(bo.at[0], dybuf.at[slot], b_recv.at[slot]).wait()
        pltpu.make_async_copy(dybuf.at[slot], dy_out.at[slot], dy_sem.at[slot]).start()

        @pl.when(j >= 2)
        def _():
            wait_b_send(s)
            wait_uz(s)

        for c in range(F // chunk):
            cs = slice(c * chunk, (c + 1) * chunk)
            a, b = _gelu_pair(_dot(hbuf[slot], w1[v, :, cs]))
            ub[s, :, cs] = a.astype(BF)
            dzb[s, :, cs] = (_dot_nt(dybuf[slot], w2[v, cs, :]) * b).astype(BF)
        pltpu.make_async_copy(ub.at[s], u_out.at[slot], u_sem.at[s]).start()
        bo[s] = (dybuf[slot].astype(F32) + _dot_nt(dzb[s], w1[v])).astype(BF)
        pltpu.make_async_copy(dzb.at[s], dz_out.at[slot], dz_sem.at[s]).start()

        final = first & (v == 0)

        @pl.when(final)
        def _():
            pltpu.make_async_copy(bo.at[s], r_out.at[m], b_send.at[s]).start()

        @pl.when(jnp.logical_not(final))
        def _():
            to = slot - jnp.where(first, M, 0)
            pltpu.make_async_remote_copy(
                src_ref=bo.at[s], dst_ref=dybuf.at[to], send_sem=b_send.at[s], recv_sem=b_recv.at[to],
                device_id={'stage': prv}, device_id_type=MESH).start()

    lead = LEAD * G // GROUP + STEP * (S - 1 - p)

    def step(k, carry):
        @pl.when(k < n)
        def _():
            forward(k)

        @pl.when(k >= lead)
        def _():
            backward(k - lead)

        return carry

    lax.fori_loop(0, n + lead, step, 0)

    for s in range(2):
        wait_f_send(s)
        wait_b_send(s)
        wait_uz(s)

    def drain(slot, carry):
        pltpu.make_async_copy(hbuf.at[slot], h_out.at[slot], h_sem.at[slot]).wait()
        pltpu.make_async_copy(dybuf.at[slot], dy_out.at[slot], dy_sem.at[slot]).wait()
        return carry

    lax.fori_loop(0, n, drain, 0)


def solution(mesh):
    S = mesh.shape['stage']

    def body(x, g, w1, w2):
        M, B, D = x.shape
        V, _, _, F = w1.shape
        w1 = w1[:, 0]
        w2 = w2[:, 0]
        G = min(GROUP, M)
        n = V * M
        p = lax.axis_index('stage')
        anys = pl.BlockSpec(memory_space=pl.ANY)
        dma = pltpu.SemaphoreType.DMA
        u, dz, h, dy, r = pl.pallas_call(
            functools.partial(_pipeline, S, V, M, G),
            out_shape=[
                jax.ShapeDtypeStruct((n, B, F), BF),
                jax.ShapeDtypeStruct((n, B, F), BF),
                jax.ShapeDtypeStruct((n, B, D), BF),
                jax.ShapeDtypeStruct((n, B, D), BF),
                jax.ShapeDtypeStruct((M, B, D), BF),
            ],
            in_specs=[anys] * 4,
            out_specs=[anys] * 5,
            scratch_shapes=[
                pltpu.VMEM((V, D, F), BF),
                pltpu.VMEM((V, F, D), BF),
                pltpu.VMEM((n, B, D), BF),
                pltpu.VMEM((n, B, D), BF),
                pltpu.VMEM((B, F), BF),
                pltpu.VMEM((2, B, F), BF),
                pltpu.VMEM((2, B, F), BF),
                pltpu.VMEM((2, B, D), BF),
                pltpu.VMEM((2, B, D), BF),
                dma((n,)), dma((n,)), dma((2,)), dma((2,)),
                dma((n,)), dma((n,)), dma((2,)), dma((2,)), dma((2 * V,)),
            ],
            compiler_params=pltpu.CompilerParams(
                collective_id=0, has_side_effects=True, vmem_limit_bytes=62 * 2 ** 20),
            cost_estimate=pl.CostEstimate(
                flops=10 * n * B * D * F, bytes_accessed=4 * n * B * F, transcendentals=3 * n * B * F),
            name='pipeline',
        )(x, g, w1, w2)

        tn = (((1,), (1,)), ((0,), (0,)))
        h = h.reshape(V, M * B, D)
        dz = dz.reshape(V, M * B, F)
        u = u.reshape(V, M * B, F)
        dy = dy.reshape(V, M * B, D)
        d1 = lax.dot_general(h, dz, tn, preferred_element_type=F32)
        d2 = lax.dot_general(u, dy, tn, preferred_element_type=F32)

        if S == 4:
            near = lax.ppermute(r, 'stage', [(0, 1), (3, 2)])
            far = lax.ppermute(r, 'stage', [(0, 2), (3, 1)])
            back = lax.ppermute(far, 'stage', [(1, 0), (2, 3)])
            y = jnp.where(p == 0, back, jnp.where(p == 1, far, jnp.where(p == 2, near, r)))
            dx = jnp.where(p == 0, r, jnp.where(p == 1, near, jnp.where(p == 2, far, back)))
        return y, dx, d1[:, None], d2[:, None]

    act = P('data', None, None)
    wsp = P(None, 'stage', None, None)
    gsp = P('data', 'stage', None, None)
    return jax.shard_map(body, mesh=mesh, in_specs=(act, act, wsp, wsp), out_specs=(act, act, gsp, gsp), check_vma=False)
```

```python
import functools

import jax
import jax.numpy as jnp
from jax import lax
from jax.experimental import pallas as pl
from jax.experimental.pallas import tpu as pltpu
from jax.sharding import PartitionSpec as P

BF = jnp.bfloat16
F32 = jnp.float32
MESH = pl.DeviceIdType.MESH
NT = (((1,), (1,)), ((), ()))
GROUP = 8
ORDER = (
    'FFFFFFFFFFFFFFFFFFFFFFFBFBBBBFBFBFBFBFBFBFBFBBBBBBBBBBBBBBBBBBBB',
    'FFFFFFFFFFFFFFFFFFFBFBFBFBFBFBBFBFBFBFBFBFBFBFBBBBBBBBBBBBBBBBBB',
    'FFFFFFFFFFFBFFBFBFBFBFBFBFBFBFBFBFBFBFBFBFBFBFBFBFBFBBBBBBBBBBBB',
    'FFFFFFFFBBBFBBFBFBFBBFFFBFBFBFBFBFBFBBFBFBFBFBFBFBFBBBBBFBBBBFFF',
)
WORD = 16


def _gelu(z):
    return 0.5 * z * (1.0 + lax.erf(z * 0.7071067811865476))


def _gelu_pair(z):
    half = 0.5 * (1.0 + lax.erf(z * 0.7071067811865476))
    return z * half, half + z * jnp.exp(-0.5 * z * z) * 0.3989422804014327


def _dot(a, b):
    return jnp.dot(a, b, preferred_element_type=F32)


def _dot_nt(a, b):
    return lax.dot_general(a, b, NT, preferred_element_type=F32)


def _words(row):
    return [sum((c == 'B') << b for b, c in enumerate(row[k:k + WORD])) for k in range(0, len(row), WORD)]


def _pipeline(S, V, M, G, x, g, w1_hbm, w2_hbm, u_out, dz_out, h_out, dy_out, mine, other,
              w1, w2, hbuf, dybuf, us, ub, dzb, fo, bo,
              f_recv, b_recv, f_send, b_send, h_sem, dy_sem, u_sem, dz_sem, w_sem, pair_send, pair_recv):
    p = lax.axis_index('stage')
    nxt = lax.rem(p + 1, S)
    prv = lax.rem(p + S - 1, S)
    parity = lax.rem(p, 2)
    partner = p + 1 - 2 * parity
    first = p == 0
    last = p == S - 1
    n = V * M
    H = M // 2
    F = w1.shape[-1]
    chunk = 256 if F % 256 == 0 else F

    barrier = pltpu.get_barrier_semaphore()
    for q in (prv, nxt):
        pl.semaphore_signal(barrier, inc=1, device_id={'stage': q}, device_id_type=MESH)

    def load_w(v):
        pltpu.make_async_copy(w1_hbm.at[v], w1.at[v], w_sem.at[2 * v]).start()
        pltpu.make_async_copy(w2_hbm.at[v], w2.at[v], w_sem.at[2 * v + 1]).start()

    def wait_w(v):
        pltpu.make_async_copy(w1_hbm.at[v], w1.at[v], w_sem.at[2 * v]).wait()
        pltpu.make_async_copy(w2_hbm.at[v], w2.at[v], w_sem.at[2 * v + 1]).wait()

    def load_x(m):
        pltpu.make_async_copy(x.at[m], hbuf.at[m], f_recv.at[m]).start()

    def load_g(m):
        s = (V - 1) * M + m
        pltpu.make_async_copy(g.at[m], dybuf.at[s], b_recv.at[s]).start()

    @pl.when(first)
    def _():
        load_x(0)

    load_w(0)

    @pl.when(first)
    def _():
        lax.fori_loop(1, M, lambda m, c: (load_x(m), c)[1], 0)

    for v in range(1, V):
        load_w(v)

    @pl.when(last)
    def _():
        lax.fori_loop(0, M, lambda m, c: (load_g(m), c)[1], 0)

    pl.semaphore_wait(barrier, 2)
    wait_w(0)

    def place(i):
        blk, r = i // (V * G), lax.rem(i, V * G)
        return r // G, blk * G + lax.rem(r, G)

    def place_f(i):
        v, m = place(i)
        early = i < G + G // 2
        v = jnp.where(last, jnp.where(i < G, 0, jnp.where(early, 1, jnp.where(i < 2 * G + G // 2, 0, 1))), v)
        m = jnp.where(last, jnp.where(i < G, i, jnp.where(early, i - G, jnp.where(i < 2 * G + G // 2, i - G // 2, i - 2 * G))), m)
        return v, m

    def wait_f_send(i):
        s = lax.rem(i, 2)
        pltpu.make_async_copy(fo.at[s], mine.at[0], f_send.at[s]).wait()

        @pl.when(last & (place_f(i)[0] == V - 1))
        def _():
            pltpu.make_async_copy(fo.at[s], mine.at[0], pair_send.at[s]).wait()

    def wait_b_send(j):
        s = lax.rem(j, 2)
        pltpu.make_async_copy(bo.at[s], mine.at[0], b_send.at[s]).wait()

        @pl.when(first & (place(j)[0] == V - 1))
        def _():
            pltpu.make_async_copy(bo.at[s], mine.at[0], pair_send.at[s]).wait()

    def wait_uz(s):
        pltpu.make_async_copy(ub.at[s], u_out.at[0], u_sem.at[s]).wait()
        pltpu.make_async_copy(dzb.at[s], dz_out.at[0], dz_sem.at[s]).wait()

    def take_h(slot):
        pltpu.make_async_copy(fo.at[0], hbuf.at[slot], f_recv.at[slot]).wait()
        pltpu.make_async_copy(hbuf.at[slot], h_out.at[slot], h_sem.at[slot]).start()

    def finish(src, s, m, sem):
        k = lax.rem(m, H)
        upper = m // H
        own = upper == parity

        def send(here, there):
            pltpu.make_async_copy(src.at[s], here.at[k], sem.at[s]).start()
            pltpu.make_async_remote_copy(
                src_ref=src.at[s], dst_ref=there.at[k], send_sem=pair_send.at[s], recv_sem=pair_recv.at[m],
                device_id={'stage': partner}, device_id_type=MESH).start()

        @pl.when(own)
        def _():
            send(mine, other)

        @pl.when(jnp.logical_not(own))
        def _():
            send(other, mine)

    def forward(i):
        v, m = place_f(i)
        slot = v * M + m
        s = lax.rem(i, 2)
        final = last & (v == V - 1)

        @pl.when(i == G - 1)
        def _():
            for vv in range(1, V):
                wait_w(vv)

        @pl.when(jnp.logical_not(final))
        def _():
            take_h(slot)

        @pl.when(i >= 2)
        def _():
            wait_f_send(i - 2)

        for c in range(F // chunk):
            cs = slice(c * chunk, (c + 1) * chunk)
            us[:, cs] = _gelu(_dot(hbuf[slot], w1[v, :, cs])).astype(BF)
        fo[s] = (hbuf[slot].astype(F32) + _dot(us[...], w2[v])).astype(BF)

        @pl.when(final)
        def _():
            finish(fo, s, m, f_send)

        @pl.when(jnp.logical_not(final))
        def _():
            to = slot + jnp.where(last, M, 0)
            pltpu.make_async_remote_copy(
                src_ref=fo.at[s], dst_ref=hbuf.at[to], send_sem=f_send.at[s], recv_sem=f_recv.at[to],
                device_id={'stage': nxt}, device_id_type=MESH).start()

    def backward(j):
        vr, m = place(j)
        v = V - 1 - vr
        slot = v * M + m
        s = lax.rem(j, 2)

        @pl.when(last & (v == V - 1))
        def _():
            take_h(slot)

        pltpu.make_async_copy(bo.at[0], dybuf.at[slot], b_recv.at[slot]).wait()
        pltpu.make_async_copy(dybuf.at[slot], dy_out.at[slot], dy_sem.at[slot]).start()

        @pl.when(j >= 2)
        def _():
            wait_b_send(j - 2)
            wait_uz(s)

        for c in range(F // chunk):
            cs = slice(c * chunk, (c + 1) * chunk)
            a, b = _gelu_pair(_dot(hbuf[slot], w1[v, :, cs]))
            ub[s, :, cs] = a.astype(BF)
            dzb[s, :, cs] = (_dot_nt(dybuf[slot], w2[v, cs, :]) * b).astype(BF)
        pltpu.make_async_copy(ub.at[s], u_out.at[slot], u_sem.at[s]).start()
        bo[s] = (dybuf[slot].astype(F32) + _dot_nt(dzb[s], w1[v])).astype(BF)
        pltpu.make_async_copy(dzb.at[s], dz_out.at[slot], dz_sem.at[s]).start()

        final = first & (v == 0)

        @pl.when(final)
        def _():
            finish(bo, s, m, b_send)

        @pl.when(jnp.logical_not(final))
        def _():
            to = slot - jnp.where(first, M, 0)
            pltpu.make_async_remote_copy(
                src_ref=bo.at[s], dst_ref=dybuf.at[to], send_sem=b_send.at[s], recv_sem=b_recv.at[to],
                device_id={'stage': prv}, device_id_type=MESH).start()

    table = [_words(row) for row in ORDER]

    def word(k):
        out = jnp.int32(0)
        for q in range(S):
            for b in range(2 * n // WORD):
                out = jnp.where((p == q) & (k == b), table[q][b], out)
        return out

    def step(t, carry):
        i, j, bits = carry
        bits = jnp.where(lax.rem(t, WORD) == 0, word(t // WORD), bits)
        back = lax.rem(bits, 2)

        @pl.when(back == 0)
        def _():
            forward(i)

        @pl.when(back == 1)
        def _():
            backward(j)

        return i + 1 - back, j + back, bits // 2

    zero = jnp.int32(0)
    lax.fori_loop(0, 2 * n, step, (zero, zero, zero))

    for k in (n - 2, n - 1):
        wait_f_send(jnp.int32(k))
        wait_b_send(jnp.int32(k))
        wait_uz(k % 2)

    def drain(slot, carry):
        pltpu.make_async_copy(hbuf.at[slot], h_out.at[slot], h_sem.at[slot]).wait()
        pltpu.make_async_copy(dybuf.at[slot], dy_out.at[slot], dy_sem.at[slot]).wait()
        return carry

    lax.fori_loop(0, n, drain, 0)

    @pl.when(jnp.logical_not(first | last))
    def _():
        lax.fori_loop(
            0, M, lambda m, c: (pltpu.make_async_copy(fo.at[0], mine.at[0], pair_recv.at[m]).wait(), c)[1], 0)


def _grad_kernel(a, b, *rest):
    rest[-1][0] = lax.dot_general(a[0], b[0], (((0,), (0,)), ((), ())), preferred_element_type=F32)


def _grad(name, a, b, wide, layers, into=None):
    V, T, A = a.shape
    N = b.shape[-1]
    lo, cnt = layers
    block = 512 if max(A, N) % 512 == 0 else max(A, N)
    nb = (A if wide == 0 else N) // block
    if wide == 0:
        specs = [pl.BlockSpec((1, T, block), lambda v, i: (v + lo, 0, i)), pl.BlockSpec((1, T, N), lambda v, i: (v + lo, 0, 0))]
        out = pl.BlockSpec((1, block, N), lambda v, i: (v + lo, i, 0))
    else:
        specs = [pl.BlockSpec((1, T, A), lambda v, i: (v + lo, 0, 0)), pl.BlockSpec((1, T, block), lambda v, i: (v + lo, 0, i))]
        out = pl.BlockSpec((1, A, block), lambda v, i: (v + lo, 0, i))
    args = [a, b]
    alias = {}
    if into is not None:
        args.append(into)
        specs.append(pl.BlockSpec(memory_space=pl.ANY))
        alias = {2: 0}
    return pl.pallas_call(
        _grad_kernel,
        grid=(cnt, nb),
        out_shape=jax.ShapeDtypeStruct((V, A, N), F32),
        in_specs=specs,
        out_specs=out,
        input_output_aliases=alias,
        compiler_params=pltpu.CompilerParams(vmem_limit_bytes=48 * 2 ** 20),
        cost_estimate=pl.CostEstimate(
            flops=2 * cnt * T * A * N, bytes_accessed=cnt * (2 * T * (A + N) + 4 * A * N), transcendentals=0),
        name=name,
    )(*args)


def _assemble(S, M, mine, other, far, back, y, dx, sem):
    p = lax.axis_index('stage')
    parity = lax.rem(p, 2)
    left = p < S // 2
    H = M // 2

    def put(src, k, dst, upper):
        pltpu.make_async_copy(src, dst.at[pl.ds(upper * H, H)], sem.at[k]).start()

    for k, src in enumerate((mine, other, far, back)):
        upper = parity if k % 2 == 0 else 1 - parity
        to_dx = left if k < 2 else jnp.logical_not(left)

        @pl.when(to_dx)
        def _():
            put(src, k, dx, upper)

        @pl.when(jnp.logical_not(to_dx))
        def _():
            put(src, k, y, upper)

    for k in range(4):
        pltpu.make_async_copy(mine, y.at[pl.ds(0, H)], sem.at[k]).wait()


def solution(mesh):
    S = mesh.shape['stage']

    def body(x, g, w1, w2):
        M, B, D = x.shape
        V, _, _, F = w1.shape
        w1 = w1[:, 0]
        w2 = w2[:, 0]
        G = GROUP
        n = V * M
        anys = pl.BlockSpec(memory_space=pl.ANY)
        dma = pltpu.SemaphoreType.DMA
        half = jax.ShapeDtypeStruct((M // 2, B, D), BF)
        u, dz, h, dy, mine, other = pl.pallas_call(
            functools.partial(_pipeline, S, V, M, G),
            out_shape=[
                jax.ShapeDtypeStruct((n, B, F), BF),
                jax.ShapeDtypeStruct((n, B, F), BF),
                jax.ShapeDtypeStruct((n, B, D), BF),
                jax.ShapeDtypeStruct((n, B, D), BF),
                half, half,
            ],
            in_specs=[anys] * 4,
            out_specs=[anys] * 6,
            scratch_shapes=[
                pltpu.VMEM((V, D, F), BF),
                pltpu.VMEM((V, F, D), BF),
                pltpu.VMEM((n, B, D), BF),
                pltpu.VMEM((n, B, D), BF),
                pltpu.VMEM((B, F), BF),
                pltpu.VMEM((2, B, F), BF),
                pltpu.VMEM((2, B, F), BF),
                pltpu.VMEM((2, B, D), BF),
                pltpu.VMEM((2, B, D), BF),
                dma((n,)), dma((n,)), dma((2,)), dma((2,)),
                dma((n,)), dma((n,)), dma((2,)), dma((2,)), dma((2 * V,)), dma((2,)), dma((M,)),
            ],
            compiler_params=pltpu.CompilerParams(
                collective_id=0, has_side_effects=True, vmem_limit_bytes=62 * 2 ** 20),
            cost_estimate=pl.CostEstimate(
                flops=10 * n * B * D * F, bytes_accessed=4 * n * B * F, transcendentals=3 * n * B * F),
            name='pipeline',
        )(x, g, w1, w2)

        h = h.reshape(V, M * B, D)
        dz = dz.reshape(V, M * B, F)
        u = u.reshape(V, M * B, F)
        dy = dy.reshape(V, M * B, D)

        far = lax.ppermute(mine, 'stage', [(q, (q + S // 2) % S) for q in range(S)])
        d1 = _grad('grad1', h, dz, 1, (0, V))
        d2 = _grad('grad2', u, dy, 0, (0, V - 1))
        far, d1, d2 = lax.optimization_barrier((far, d1, d2))
        back = lax.ppermute(far, 'stage', [(q, q + 1 - 2 * (q % 2)) for q in range(S)])
        d2 = _grad('grad3', u, dy, 0, (V - 1, 1), d2)
        back, d2 = lax.optimization_barrier((back, d2))
        full = jax.ShapeDtypeStruct((M, B, D), BF)
        y, dx = pl.pallas_call(
            functools.partial(_assemble, S, M),
            out_shape=[full, full],
            in_specs=[pl.BlockSpec(memory_space=pltpu.VMEM)] * 4,
            out_specs=[anys] * 2,
            scratch_shapes=[dma((4,))],
            compiler_params=pltpu.CompilerParams(vmem_limit_bytes=16 * 2 ** 20),
            name='assemble',
        )(mine, other, far, back)
        return y, dx, d1[:, None], d2[:, None]

    act = P('data', None, None)
    wsp = P(None, 'stage', None, None)
    gsp = P('data', 'stage', None, None)
    return jax.shard_map(body, mesh=mesh, in_specs=(act, act, wsp, wsp), out_specs=(act, act, gsp, gsp), check_vma=False)
```

```python
import functools

import jax
import jax.numpy as jnp
from jax import lax
from jax.experimental import pallas as pl
from jax.experimental.pallas import tpu as pltpu
from jax.sharding import PartitionSpec as P

BF = jnp.bfloat16
F32 = jnp.float32
MESH = pl.DeviceIdType.MESH
NT = (((1,), (1,)), ((), ()))
GROUP = 8
ORDER = (
    'FFFFFFFFFFFFFFFFFFFFFFFBFBBBBFBFBFBFBFBFBFBFBBBBBBBBBBBBBBBBBBBB',
    'FFFFFFFFFFFFFFFFFFFBFBFBFBFBFBBFBFBFBFBFBFBFBFBBBBBBBBBBBBBBBBBB',
    'FFFFFFFFFFFBFFBFBFBFBFBFBFBFBFBFBFBFBFBFBFBFBFBFBFBFBBBBBBBBBBBB',
    'FFFFFFFFBBBFBBFBFBFBBFFFBFBFBFBFBFBFBBFBFBFBFBFBFBFBBBBBFBBBBFFF',
)
WORD = 16


def _gelu(z):
    return 0.5 * z * (1.0 + lax.erf(z * 0.7071067811865476))


def _gelu_pair(z):
    half = 0.5 * (1.0 + lax.erf(z * 0.7071067811865476))
    return z * half, half + z * jnp.exp(-0.5 * z * z) * 0.3989422804014327


def _dot(a, b):
    return jnp.dot(a, b, preferred_element_type=F32)


def _dot_nt(a, b):
    return lax.dot_general(a, b, NT, preferred_element_type=F32)


def _words(row):
    return [sum((c == 'B') << b for b, c in enumerate(row[k:k + WORD])) for k in range(0, len(row), WORD)]


def _pipeline(S, V, M, G, x, g, w1_hbm, w2_hbm, u_out, dz_out, h_out, dy_out, mine, other,
              w1, w2, hbuf, dybuf, us, ub, dzb, fo, bo,
              f_recv, b_recv, f_send, b_send, h_sem, dy_sem, u_sem, dz_sem, w_sem, pair_send, pair_recv):
    p = lax.axis_index('stage')
    nxt = lax.rem(p + 1, S)
    prv = lax.rem(p + S - 1, S)
    parity = lax.rem(p, 2)
    partner = p + 1 - 2 * parity
    first = p == 0
    last = p == S - 1
    n = V * M
    H = M // 2
    F = w1.shape[-1]
    chunk = 256 if F % 256 == 0 else F

    barrier = pltpu.get_barrier_semaphore()
    for q in (prv, nxt):
        pl.semaphore_signal(barrier, inc=1, device_id={'stage': q}, device_id_type=MESH)

    def load_w(v):
        pltpu.make_async_copy(w1_hbm.at[v], w1.at[v], w_sem.at[2 * v]).start()
        pltpu.make_async_copy(w2_hbm.at[v], w2.at[v], w_sem.at[2 * v + 1]).start()

    def wait_w(v):
        pltpu.make_async_copy(w1_hbm.at[v], w1.at[v], w_sem.at[2 * v]).wait()
        pltpu.make_async_copy(w2_hbm.at[v], w2.at[v], w_sem.at[2 * v + 1]).wait()

    def load_x(m):
        pltpu.make_async_copy(x.at[m], hbuf.at[m], f_recv.at[m]).start()

    def load_g(m):
        s = (V - 1) * M + m
        pltpu.make_async_copy(g.at[m], dybuf.at[s], b_recv.at[s]).start()

    @pl.when(first)
    def _():
        load_x(0)

    load_w(0)

    @pl.when(first)
    def _():
        lax.fori_loop(1, M, lambda m, c: (load_x(m), c)[1], 0)

    for v in range(1, V):
        load_w(v)

    @pl.when(last)
    def _():
        lax.fori_loop(0, M, lambda m, c: (load_g(m), c)[1], 0)

    pl.semaphore_wait(barrier, 2)
    wait_w(0)

    def place(i):
        blk, r = i // (V * G), lax.rem(i, V * G)
        return r // G, blk * G + lax.rem(r, G)

    def place_f(i):
        v, m = place(i)
        early = i < G + G // 2
        v = jnp.where(last, jnp.where(i < G, 0, jnp.where(early, 1, jnp.where(i < 2 * G + G // 2, 0, 1))), v)
        m = jnp.where(last, jnp.where(i < G, i, jnp.where(early, i - G, jnp.where(i < 2 * G + G // 2, i - G // 2, i - 2 * G))), m)
        return v, m

    def wait_f_send(i):
        s = lax.rem(i, 2)
        pltpu.make_async_copy(fo.at[s], mine.at[0], f_send.at[s]).wait()

        @pl.when(last & (place_f(i)[0] == V - 1))
        def _():
            pltpu.make_async_copy(fo.at[s], mine.at[0], pair_send.at[s]).wait()

    def wait_b_send(j):
        s = lax.rem(j, 2)
        pltpu.make_async_copy(bo.at[s], mine.at[0], b_send.at[s]).wait()

        @pl.when(first & (place(j)[0] == V - 1))
        def _():
            pltpu.make_async_copy(bo.at[s], mine.at[0], pair_send.at[s]).wait()

    def wait_uz(s):
        pltpu.make_async_copy(ub.at[s], u_out.at[0], u_sem.at[s]).wait()
        pltpu.make_async_copy(dzb.at[s], dz_out.at[0], dz_sem.at[s]).wait()

    def take_h(slot):
        pltpu.make_async_copy(fo.at[0], hbuf.at[slot], f_recv.at[slot]).wait()
        pltpu.make_async_copy(hbuf.at[slot], h_out.at[slot], h_sem.at[slot]).start()

    def finish(src, s, m, sem):
        k = lax.rem(m, H)
        upper = m // H
        own = upper == parity

        def send(here, there):
            pltpu.make_async_copy(src.at[s], here.at[k], sem.at[s]).start()
            pltpu.make_async_remote_copy(
                src_ref=src.at[s], dst_ref=there.at[k], send_sem=pair_send.at[s], recv_sem=pair_recv.at[m],
                device_id={'stage': partner}, device_id_type=MESH).start()

        @pl.when(own)
        def _():
            send(mine, other)

        @pl.when(jnp.logical_not(own))
        def _():
            send(other, mine)

    def forward(i):
        v, m = place_f(i)
        slot = v * M + m
        s = lax.rem(i, 2)
        final = last & (v == V - 1)

        @pl.when(i == G - 1)
        def _():
            for vv in range(1, V):
                wait_w(vv)

        @pl.when(jnp.logical_not(final))
        def _():
            take_h(slot)

        @pl.when(i >= 2)
        def _():
            wait_f_send(i - 2)

        for c in range(F // chunk):
            cs = slice(c * chunk, (c + 1) * chunk)
            us[:, cs] = _gelu(_dot(hbuf[slot], w1[v, :, cs])).astype(BF)
        fo[s] = (hbuf[slot].astype(F32) + _dot(us[...], w2[v])).astype(BF)

        @pl.when(final)
        def _():
            finish(fo, s, m, f_send)

        @pl.when(jnp.logical_not(final))
        def _():
            to = slot + jnp.where(last, M, 0)
            pltpu.make_async_remote_copy(
                src_ref=fo.at[s], dst_ref=hbuf.at[to], send_sem=f_send.at[s], recv_sem=f_recv.at[to],
                device_id={'stage': nxt}, device_id_type=MESH).start()

    def backward(j):
        vr, m = place(j)
        v = V - 1 - vr
        slot = v * M + m
        s = lax.rem(j, 2)

        @pl.when(last & (v == V - 1))
        def _():
            take_h(slot)

        pltpu.make_async_copy(bo.at[0], dybuf.at[slot], b_recv.at[slot]).wait()
        pltpu.make_async_copy(dybuf.at[slot], dy_out.at[slot], dy_sem.at[slot]).start()

        @pl.when(j >= 2)
        def _():
            wait_b_send(j - 2)
            wait_uz(s)

        for c in range(F // chunk):
            cs = slice(c * chunk, (c + 1) * chunk)
            a, b = _gelu_pair(_dot(hbuf[slot], w1[v, :, cs]))
            ub[s, :, cs] = a.astype(BF)
            dzb[s, :, cs] = (_dot_nt(dybuf[slot], w2[v, cs, :]) * b).astype(BF)
        pltpu.make_async_copy(ub.at[s], u_out.at[slot], u_sem.at[s]).start()
        bo[s] = (dybuf[slot].astype(F32) + _dot_nt(dzb[s], w1[v])).astype(BF)
        pltpu.make_async_copy(dzb.at[s], dz_out.at[slot], dz_sem.at[s]).start()

        final = first & (v == 0)

        @pl.when(final)
        def _():
            finish(bo, s, m, b_send)

        @pl.when(jnp.logical_not(final))
        def _():
            to = slot - jnp.where(first, M, 0)
            pltpu.make_async_remote_copy(
                src_ref=bo.at[s], dst_ref=dybuf.at[to], send_sem=b_send.at[s], recv_sem=b_recv.at[to],
                device_id={'stage': prv}, device_id_type=MESH).start()

    table = [_words(row) for row in ORDER]

    def word(k):
        out = jnp.int32(0)
        for q in range(S):
            for b in range(2 * n // WORD):
                out = jnp.where((p == q) & (k == b), table[q][b], out)
        return out

    def step(t, carry):
        i, j, bits = carry
        bits = jnp.where(lax.rem(t, WORD) == 0, word(t // WORD), bits)
        back = lax.rem(bits, 2)

        @pl.when(back == 0)
        def _():
            forward(i)

        @pl.when(back == 1)
        def _():
            backward(j)

        return i + 1 - back, j + back, bits // 2

    zero = jnp.int32(0)
    lax.fori_loop(0, 2 * n, step, (zero, zero, zero))

    for k in (n - 2, n - 1):
        wait_f_send(jnp.int32(k))
        wait_b_send(jnp.int32(k))
        wait_uz(k % 2)

    def drain(slot, carry):
        pltpu.make_async_copy(hbuf.at[slot], h_out.at[slot], h_sem.at[slot]).wait()
        pltpu.make_async_copy(dybuf.at[slot], dy_out.at[slot], dy_sem.at[slot]).wait()
        return carry

    lax.fori_loop(0, n, drain, 0)

    @pl.when(jnp.logical_not(first | last))
    def _():
        lax.fori_loop(
            0, M, lambda m, c: (pltpu.make_async_copy(fo.at[0], mine.at[0], pair_recv.at[m]).wait(), c)[1], 0)


def _grads(phases, block, pieces, h, dz, u, dy, *rest):
    d1, d2, narrow, wide, o1, o2, n_sem, w_sem, o_sem, p_sem = rest[-10:]
    T, N = wide.shape[1:]
    nb = dz.shape[-1] // block
    total = len(phases) * nb
    tn = (((0,), (0,)), ((), ()))

    def pick(s, values):
        out = jnp.int32(values[0])
        for q in range(1, len(values)):
            out = jnp.where(s // nb == q, values[q], out)
        return out

    kinds = [k for k, _ in phases]
    layers = [v for _, v in phases]

    def narrow_copy(q, act):
        kind, v = phases[q]
        src = dy if kind else h
        act(pltpu.make_async_copy(src.at[v], narrow.at[q % 2], n_sem.at[q % 2]))

    def wide_copy(s, act):
        kind, v = pick(s, kinds), pick(s, layers)
        slot = lax.rem(s, 2)
        cols = pl.ds(pl.multiple_of(lax.rem(s, nb) * block, block), block)
        for k, src in ((0, dz), (1, u)):
            if k in kinds:
                @pl.when(kind == k)
                def _():
                    act(pltpu.make_async_copy(src.at[v, :, cols], wide.at[slot], w_sem.at[slot]))

    def out_copy(s, act):
        kind, v = pick(s, kinds), pick(s, layers)
        slot = lax.rem(s, 2)
        cols = pl.ds(pl.multiple_of(lax.rem(s, nb) * block, block), block)
        if 0 in kinds:
            @pl.when(kind == 0)
            def _():
                act(pltpu.make_async_copy(o1.at[slot], d1.at[v, :, cols], o_sem.at[slot]))
        if 1 in kinds:
            @pl.when(kind == 1)
            def _():
                act(pltpu.make_async_copy(o2.at[slot], d2.at[v, cols, :], o_sem.at[slot]))

    start = lambda c: c.start()
    wait = lambda c: c.wait()

    kind0, v0 = phases[0]
    rows = T // pieces

    def piece(r, act):
        sl = pl.ds(r * rows, rows)
        act(pltpu.make_async_copy((dy if kind0 else h).at[v0, sl], narrow.at[0, sl], p_sem.at[2 * r]))
        act(pltpu.make_async_copy((u if kind0 else dz).at[v0, sl, pl.ds(0, block)], wide.at[0, sl], p_sem.at[2 * r + 1]))

    for r in range(pieces):
        piece(r, start)
    wide_copy(jnp.int32(1), start)
    if len(phases) > 1:
        narrow_copy(1, start)

    for r in range(pieces):
        piece(r, wait)
        sl = slice(r * rows, (r + 1) * rows)
        if kind0:
            part = lax.dot_general(wide[0, sl], narrow[0, sl], tn, preferred_element_type=F32)
            o2[0] = part if r == 0 else o2[0] + part
        else:
            part = lax.dot_general(narrow[0, sl], wide[0, sl], tn, preferred_element_type=F32)
            o1[0] = part if r == 0 else o1[0] + part
    out_copy(jnp.int32(0), start)

    def step(s, carry):
        slot = lax.rem(s, 2)
        kind = pick(s, kinds)
        side = lax.rem(s // nb, 2)
        wide_copy(s, wait)
        for q in range(1, len(phases)):
            @pl.when(s == q * nb)
            def _():
                narrow_copy(q, wait)
                if q + 1 < len(phases):
                    narrow_copy(q + 1, start)

        @pl.when(s + 1 < total)
        def _():
            wide_copy(s + 1, start)

        @pl.when(s >= 2)
        def _():
            out_copy(s - 2, wait)

        if 0 in kinds:
            @pl.when(kind == 0)
            def _():
                o1[slot] = lax.dot_general(narrow[side], wide[slot], tn, preferred_element_type=F32)
        if 1 in kinds:
            @pl.when(kind == 1)
            def _():
                o2[slot] = lax.dot_general(wide[slot], narrow[side], tn, preferred_element_type=F32)
        out_copy(s, start)
        return carry

    lax.fori_loop(1, total, step, jnp.int32(0))
    for s in (total - 2, total - 1):
        out_copy(jnp.int32(s), wait)


def _grad(name, phases, h, dz, u, dy, into=None):
    V, T, D = h.shape
    F = dz.shape[-1]
    block = 1024 if F % 1024 == 0 else F // 2
    dma = pltpu.SemaphoreType.DMA
    pieces = 4
    args = [h, dz, u, dy] + list(into or ())
    return pl.pallas_call(
        functools.partial(_grads, phases, block, pieces),
        out_shape=[jax.ShapeDtypeStruct((V, D, F), F32), jax.ShapeDtypeStruct((V, F, D), F32)],
        in_specs=[pl.BlockSpec(memory_space=pl.ANY)] * len(args),
        out_specs=[pl.BlockSpec(memory_space=pl.ANY)] * 2,
        scratch_shapes=[
            pltpu.VMEM((2, T, D), BF),
            pltpu.VMEM((2, T, block), BF),
            pltpu.VMEM((2, D, block), F32),
            pltpu.VMEM((2, block, D), F32),
            dma((2,)), dma((2,)), dma((2,)), dma((2 * pieces,)),
        ],
        input_output_aliases={4: 0, 5: 1} if into else {},
        compiler_params=pltpu.CompilerParams(vmem_limit_bytes=54 * 2 ** 20),
        cost_estimate=pl.CostEstimate(
            flops=2 * len(phases) * T * D * F, bytes_accessed=len(phases) * (2 * T * (D + F) + 4 * D * F), transcendentals=0),
        name=name,
    )(*args)


def _assemble(S, M, mine, other, far, back, y, dx, sem):
    p = lax.axis_index('stage')
    parity = lax.rem(p, 2)
    left = p < S // 2
    H = M // 2

    def put(src, k, dst, upper):
        pltpu.make_async_copy(src, dst.at[pl.ds(upper * H, H)], sem.at[k]).start()

    for k, src in enumerate((mine, other, far, back)):
        upper = parity if k % 2 == 0 else 1 - parity
        to_dx = left if k < 2 else jnp.logical_not(left)

        @pl.when(to_dx)
        def _():
            put(src, k, dx, upper)

        @pl.when(jnp.logical_not(to_dx))
        def _():
            put(src, k, y, upper)

    for k in range(4):
        pltpu.make_async_copy(mine, y.at[pl.ds(0, H)], sem.at[k]).wait()


def solution(mesh):
    S = mesh.shape['stage']

    def body(x, g, w1, w2):
        M, B, D = x.shape
        V, _, _, F = w1.shape
        w1 = w1[:, 0]
        w2 = w2[:, 0]
        G = GROUP
        n = V * M
        anys = pl.BlockSpec(memory_space=pl.ANY)
        dma = pltpu.SemaphoreType.DMA
        half = jax.ShapeDtypeStruct((M // 2, B, D), BF)
        u, dz, h, dy, mine, other = pl.pallas_call(
            functools.partial(_pipeline, S, V, M, G),
            out_shape=[
                jax.ShapeDtypeStruct((n, B, F), BF),
                jax.ShapeDtypeStruct((n, B, F), BF),
                jax.ShapeDtypeStruct((n, B, D), BF),
                jax.ShapeDtypeStruct((n, B, D), BF),
                half, half,
            ],
            in_specs=[anys] * 4,
            out_specs=[anys] * 6,
            scratch_shapes=[
                pltpu.VMEM((V, D, F), BF),
                pltpu.VMEM((V, F, D), BF),
                pltpu.VMEM((n, B, D), BF),
                pltpu.VMEM((n, B, D), BF),
                pltpu.VMEM((B, F), BF),
                pltpu.VMEM((2, B, F), BF),
                pltpu.VMEM((2, B, F), BF),
                pltpu.VMEM((2, B, D), BF),
                pltpu.VMEM((2, B, D), BF),
                dma((n,)), dma((n,)), dma((2,)), dma((2,)),
                dma((n,)), dma((n,)), dma((2,)), dma((2,)), dma((2 * V,)), dma((2,)), dma((M,)),
            ],
            compiler_params=pltpu.CompilerParams(
                collective_id=0, has_side_effects=True, vmem_limit_bytes=62 * 2 ** 20),
            cost_estimate=pl.CostEstimate(
                flops=10 * n * B * D * F, bytes_accessed=4 * n * B * F, transcendentals=3 * n * B * F),
            name='pipeline',
        )(x, g, w1, w2)

        h = h.reshape(V, M * B, D)
        dz = dz.reshape(V, M * B, F)
        u = u.reshape(V, M * B, F)
        dy = dy.reshape(V, M * B, D)

        far = lax.ppermute(mine, 'stage', [(q, (q + S // 2) % S) for q in range(S)])
        todo = [(0, v) for v in range(V)] + [(1, v) for v in range(V)]
        d1, d2 = _grad('grads', todo[:-1], h, dz, u, dy)
        far, d1, d2 = lax.optimization_barrier((far, d1, d2))
        back = lax.ppermute(far, 'stage', [(q, q + 1 - 2 * (q % 2)) for q in range(S)])
        d1, d2 = _grad('grads_last', todo[-1:], h, dz, u, dy, (d1, d2))
        back, d1, d2 = lax.optimization_barrier((back, d1, d2))
        full = jax.ShapeDtypeStruct((M, B, D), BF)
        y, dx = pl.pallas_call(
            functools.partial(_assemble, S, M),
            out_shape=[full, full],
            in_specs=[pl.BlockSpec(memory_space=pltpu.VMEM)] * 4,
            out_specs=[anys] * 2,
            scratch_shapes=[dma((4,))],
            compiler_params=pltpu.CompilerParams(vmem_limit_bytes=16 * 2 ** 20),
            name='assemble',
        )(mine, other, far, back)
        return y, dx, d1[:, None], d2[:, None]

    act = P('data', None, None)
    wsp = P(None, 'stage', None, None)
    gsp = P('data', 'stage', None, None)
    return jax.shard_map(body, mesh=mesh, in_specs=(act, act, wsp, wsp), out_specs=(act, act, gsp, gsp), check_vma=False)
```

```python
import functools

import jax
import jax.numpy as jnp
from jax import lax
from jax.experimental import pallas as pl
from jax.experimental.pallas import tpu as pltpu
from jax.sharding import PartitionSpec as P

BF = jnp.bfloat16
F32 = jnp.float32
MESH = pl.DeviceIdType.MESH
NT = (((1,), (1,)), ((), ()))
GROUP = 8
ORDER = (
    'FFFFFFFFFFFFFFFFFFFFFBFBFBBBFMMMBFFMMBMBBBBBBBBBBBBBBBBBBB',
    'FFFFFFFFFFFFFFFFFMFBFMBBFBFMBMFBFMFBFBFBMBBBBBBBBBBBBBBBBB',
    'FFFFFFFFFFFMFMBMMMMMMMMMMMMMMFBMMMBBBBBBBBBBB',
    'FFFFFFFFBBBBFFBBFBMMMMMMMMMMMMMMMMMBBBMBBBBFFF',
)
WORD = 15


def _gelu(z):
    return 0.5 * z * (1.0 + lax.erf(z * 0.7071067811865476))


def _gelu_pair(z):
    half = 0.5 * (1.0 + lax.erf(z * 0.7071067811865476))
    return z * half, half + z * jnp.exp(-0.5 * z * z) * 0.3989422804014327


def _dot(a, b):
    return jnp.dot(a, b, preferred_element_type=F32)


def _dot_nt(a, b):
    return lax.dot_general(a, b, NT, preferred_element_type=F32)


def _words(row):
    return [sum('FBM'.index(c) * 4 ** b for b, c in enumerate(row[k:k + WORD])) for k in range(0, len(row), WORD)]


def _pipeline(S, V, M, G, x, g, w1_hbm, w2_hbm, u_out, dz_out, h_out, dy_out, mine, other,
              w1, w2, hbuf, dybuf, us, ub, dzb, fo, bo,
              f_recv, b_recv, f_send, b_send, h_sem, dy_sem, u_sem, dz_sem, w_sem, pair_send, pair_recv):
    p = lax.axis_index('stage')
    nxt = lax.rem(p + 1, S)
    prv = lax.rem(p + S - 1, S)
    parity = lax.rem(p, 2)
    partner = p + 1 - 2 * parity
    first = p == 0
    last = p == S - 1
    n = V * M
    H = M // 2
    F = w1.shape[-1]
    chunk = 256 if F % 256 == 0 else F

    barrier = pltpu.get_barrier_semaphore()
    for q in (prv, nxt):
        pl.semaphore_signal(barrier, inc=1, device_id={'stage': q}, device_id_type=MESH)

    def load_w(v):
        pltpu.make_async_copy(w1_hbm.at[v], w1.at[v], w_sem.at[2 * v]).start()
        pltpu.make_async_copy(w2_hbm.at[v], w2.at[v], w_sem.at[2 * v + 1]).start()

    def wait_w(v):
        pltpu.make_async_copy(w1_hbm.at[v], w1.at[v], w_sem.at[2 * v]).wait()
        pltpu.make_async_copy(w2_hbm.at[v], w2.at[v], w_sem.at[2 * v + 1]).wait()

    def load_x(m):
        pltpu.make_async_copy(x.at[m], hbuf.at[m], f_recv.at[m]).start()

    def load_g(m):
        s = (V - 1) * M + m
        pltpu.make_async_copy(g.at[m], dybuf.at[s], b_recv.at[s]).start()

    @pl.when(first)
    def _():
        load_x(0)

    load_w(0)

    @pl.when(first)
    def _():
        lax.fori_loop(1, M, lambda m, c: (load_x(m), c)[1], 0)

    for v in range(1, V):
        load_w(v)

    @pl.when(last)
    def _():
        lax.fori_loop(0, M, lambda m, c: (load_g(m), c)[1], 0)

    pl.semaphore_wait(barrier, 2)
    wait_w(0)

    def place(i):
        blk, r = i // (V * G), lax.rem(i, V * G)
        return r // G, blk * G + lax.rem(r, G)

    def place_f(i):
        v, m = place(i)
        early = i < G + G // 2
        v = jnp.where(last, jnp.where(i < G, 0, jnp.where(early, 1, jnp.where(i < 2 * G + G // 2, 0, 1))), v)
        m = jnp.where(last, jnp.where(i < G, i, jnp.where(early, i - G, jnp.where(i < 2 * G + G // 2, i - G // 2, i - 2 * G))), m)
        return v, m

    def wait_f_send(i):
        s = lax.rem(i, 2)
        pltpu.make_async_copy(fo.at[s], mine.at[0], f_send.at[s]).wait()

        @pl.when(last & (place_f(i)[0] == V - 1))
        def _():
            pltpu.make_async_copy(fo.at[s], mine.at[0], pair_send.at[s]).wait()

    def wait_b_send(j):
        s = lax.rem(j, 2)
        pltpu.make_async_copy(bo.at[s], mine.at[0], b_send.at[s]).wait()

        @pl.when(first & (place(j)[0] == V - 1))
        def _():
            pltpu.make_async_copy(bo.at[s], mine.at[0], pair_send.at[s]).wait()

    def wait_uz(s):
        pltpu.make_async_copy(ub.at[s], u_out.at[0], u_sem.at[s]).wait()
        pltpu.make_async_copy(dzb.at[s], dz_out.at[0], dz_sem.at[s]).wait()

    def take_h(slot):
        pltpu.make_async_copy(fo.at[0], hbuf.at[slot], f_recv.at[slot]).wait()
        pltpu.make_async_copy(hbuf.at[slot], h_out.at[slot], h_sem.at[slot]).start()

    def halves(m, put):
        own = m // H == parity

        @pl.when(own)
        def _():
            put(mine, other)

        @pl.when(jnp.logical_not(own))
        def _():
            put(other, mine)

    def ready_f(i):
        v, m = place_f(i)

        @pl.when(i == G - 1)
        def _():
            for vv in range(1, V):
                wait_w(vv)

        @pl.when(jnp.logical_not(last & (v == V - 1)))
        def _():
            take_h(v * M + m)

        @pl.when(i >= 2)
        def _():
            wait_f_send(i - 2)

    def compute_f(i):
        v, m = place_f(i)
        slot = v * M + m
        s = lax.rem(i, 2)
        for c in range(F // chunk):
            cs = slice(c * chunk, (c + 1) * chunk)
            us[:, cs] = _gelu(_dot(hbuf[slot], w1[v, :, cs])).astype(BF)
        fo[s] = (hbuf[slot].astype(F32) + _dot(us[...], w2[v])).astype(BF)
        to = slot + jnp.where(last, M, 0)
        pltpu.make_async_remote_copy(
            src_ref=fo.at[s], dst_ref=hbuf.at[to], send_sem=f_send.at[s], recv_sem=f_recv.at[to],
            device_id={'stage': jnp.where(last & (v == V - 1), partner, nxt)}, device_id_type=MESH).start()

    def done_f(i):
        v, m = place_f(i)
        s = lax.rem(i, 2)

        @pl.when(last & (v == V - 1))
        def _():
            halves(m, lambda here, there: pltpu.make_async_copy(
                fo.at[s], here.at[lax.rem(m, H)], pair_send.at[s]).start())

    def place_b(j):
        vr, m = place(j)
        return V - 1 - vr, m

    def ready_b(j):
        v, m = place_b(j)
        slot = v * M + m

        @pl.when(last & (v == V - 1))
        def _():
            take_h(slot)

        pltpu.make_async_copy(bo.at[0], dybuf.at[slot], b_recv.at[slot]).wait()
        pltpu.make_async_copy(dybuf.at[slot], dy_out.at[slot], dy_sem.at[slot]).start()

        @pl.when(j >= 2)
        def _():
            wait_b_send(j - 2)
            wait_uz(lax.rem(j, 2))

    def compute_b(j):
        v, m = place_b(j)
        slot = v * M + m
        s = lax.rem(j, 2)
        for c in range(F // chunk):
            cs = slice(c * chunk, (c + 1) * chunk)
            a, b = _gelu_pair(_dot(hbuf[slot], w1[v, :, cs]))
            ub[s, :, cs] = a.astype(BF)
            dzb[s, :, cs] = (_dot_nt(dybuf[slot], w2[v, cs, :]) * b).astype(BF)
        pltpu.make_async_copy(ub.at[s], u_out.at[slot], u_sem.at[s]).start()
        bo[s] = (dybuf[slot].astype(F32) + _dot_nt(dzb[s], w1[v])).astype(BF)
        pltpu.make_async_copy(dzb.at[s], dz_out.at[slot], dz_sem.at[s]).start()

    def done_b(j):
        v, m = place_b(j)
        slot = v * M + m
        s = lax.rem(j, 2)
        final = first & (v == 0)

        @pl.when(final)
        def _():
            k = lax.rem(m, H)

            def put(here, there):
                pltpu.make_async_copy(bo.at[s], here.at[k], b_send.at[s]).start()
                pltpu.make_async_remote_copy(
                    src_ref=bo.at[s], dst_ref=there.at[k], send_sem=pair_send.at[s], recv_sem=pair_recv.at[m],
                    device_id={'stage': partner}, device_id_type=MESH).start()

            halves(m, put)

        @pl.when(jnp.logical_not(final))
        def _():
            to = slot - jnp.where(first, M, 0)
            pltpu.make_async_remote_copy(
                src_ref=bo.at[s], dst_ref=dybuf.at[to], send_sem=b_send.at[s], recv_sem=b_recv.at[to],
                device_id={'stage': prv}, device_id_type=MESH).start()

    table = [_words(row) for row in ORDER]

    def word(k):
        out = jnp.int32(0)
        for q in range(S):
            for b in range(len(table[q])):
                out = jnp.where((p == q) & (k == b), table[q][b], out)
        return out

    def step(t, carry):
        i, j, bits = carry
        bits = jnp.where(lax.rem(t, WORD) == 0, word(t // WORD), bits)
        kind = lax.rem(bits, 4)

        @pl.when(kind == 0)
        def _():
            ready_f(i)
            compute_f(i)
            done_f(i)

        @pl.when(kind == 1)
        def _():
            ready_b(j)
            compute_b(j)
            done_b(j)

        @pl.when(kind == 2)
        def _():
            ready_f(i)
            ready_b(j)
            compute_f(i)
            compute_b(j)
            done_f(i)
            done_b(j)

        return i + jnp.where(kind == 1, 0, 1), j + jnp.where(kind == 0, 0, 1), bits // 4

    zero = jnp.int32(0)
    count = jnp.int32(0)
    for q in range(S):
        count = jnp.where(p == q, len(ORDER[q]), count)
    lax.fori_loop(0, count, step, (zero, zero, zero))

    for k in (n - 2, n - 1):
        wait_f_send(jnp.int32(k))
        wait_b_send(jnp.int32(k))
        wait_uz(k % 2)

    @pl.when(p == S - 2)
    def _():
        def take(m, c):
            pltpu.make_async_copy(fo.at[0], hbuf.at[n + m], f_recv.at[n + m]).wait()
            return c

        lax.fori_loop(0, M, take, 0)
        copies = [pltpu.make_async_copy(hbuf.at[pl.ds(n + k * H, H)], ref, pair_send.at[k]) for k, ref in enumerate((mine, other))]
        for c in copies:
            c.start()
        for c in copies:
            c.wait()

    def drain(slot, carry):
        pltpu.make_async_copy(hbuf.at[slot], h_out.at[slot], h_sem.at[slot]).wait()
        pltpu.make_async_copy(dybuf.at[slot], dy_out.at[slot], dy_sem.at[slot]).wait()
        return carry

    lax.fori_loop(0, n, drain, 0)

    @pl.when(p == 1)
    def _():
        lax.fori_loop(
            0, M, lambda m, c: (pltpu.make_async_copy(fo.at[0], mine.at[0], pair_recv.at[m]).wait(), c)[1], 0)


def _grads(work, block, pieces, h, dz, u, dy, *rest):
    d1, d2, narrow, wide, o1, o2, n_sem, w_sem, o_sem, p_sem = rest[-10:]
    T = wide.shape[1]
    begin = [sum(w[3] for w in work[:q]) for q in range(len(work) + 1)]
    total = begin[-1]
    tn = (((0,), (0,)), ((), ()))
    kinds = [w[0] for w in work]

    def pick(s, values):
        out = jnp.int32(values[0])
        for q in range(1, len(work)):
            out = jnp.where(s >= begin[q], values[q], out)
        return out

    def at(s):
        v = pick(s, [w[1] for w in work])
        blk = s + pick(s, [w[2] - begin[q] for q, w in enumerate(work)])
        return pick(s, kinds), v, pl.ds(pl.multiple_of(blk * block, block), block), lax.rem(s, 2)

    def narrow_copy(q, act):
        act(pltpu.make_async_copy((dy if kinds[q] else h).at[work[q][1]], narrow.at[q % 2], n_sem.at[q % 2]))

    def wide_copy(s, act):
        kind, v, cols, slot = at(s)
        for k, src in ((0, dz), (1, u)):
            if k in kinds:
                @pl.when(kind == k)
                def _():
                    act(pltpu.make_async_copy(src.at[v, :, cols], wide.at[slot], w_sem.at[slot]))

    def out_copy(s, act):
        kind, v, cols, slot = at(s)
        if 0 in kinds:
            @pl.when(kind == 0)
            def _():
                act(pltpu.make_async_copy(o1.at[slot], d1.at[v, :, cols], o_sem.at[slot]))
        if 1 in kinds:
            @pl.when(kind == 1)
            def _():
                act(pltpu.make_async_copy(o2.at[slot], d2.at[v, cols, :], o_sem.at[slot]))

    start = lambda c: c.start()
    wait = lambda c: c.wait()
    rows = T // pieces

    def piece(r, act):
        sl = pl.ds(pl.multiple_of(r * rows, rows), rows)
        act(pltpu.make_async_copy(h.at[work[0][1], sl], narrow.at[0, sl], p_sem.at[2 * r]))
        act(pltpu.make_async_copy(dz.at[work[0][1], sl, pl.ds(work[0][2] * block, block)], wide.at[0, sl], p_sem.at[2 * r + 1]))

    for r in range(pieces):
        piece(r, start)
    wide_copy(jnp.int32(1), start)
    if len(work) > 1:
        narrow_copy(1, start)

    piece(0, wait)
    o1[0] = lax.dot_general(narrow[0, :rows], wide[0, :rows], tn, preferred_element_type=F32)

    def add(r, carry):
        piece(r, wait)
        sl = pl.ds(pl.multiple_of(r * rows, rows), rows)
        o1[0] += lax.dot_general(narrow[0, sl], wide[0, sl], tn, preferred_element_type=F32)
        return carry

    lax.fori_loop(1, pieces, add, jnp.int32(0))
    out_copy(jnp.int32(0), start)

    def step(s, carry):
        kind, _, _, slot = at(s)
        side = pick(s, [q % 2 for q in range(len(work))])
        wide_copy(s, wait)
        for q in range(1, len(work)):
            @pl.when(s == begin[q])
            def _():
                narrow_copy(q, wait)
                if q + 1 < len(work):
                    narrow_copy(q + 1, start)

        @pl.when(s + 1 < total)
        def _():
            wide_copy(s + 1, start)

        @pl.when(s >= 2)
        def _():
            out_copy(s - 2, wait)

        if 0 in kinds:
            @pl.when(kind == 0)
            def _():
                o1[slot] = lax.dot_general(narrow[side], wide[slot], tn, preferred_element_type=F32)
        if 1 in kinds:
            @pl.when(kind == 1)
            def _():
                o2[slot] = lax.dot_general(wide[slot], narrow[side], tn, preferred_element_type=F32)
        out_copy(s, start)
        return carry

    lax.fori_loop(1, total, step, jnp.int32(0))
    for s in (total - 2, total - 1):
        out_copy(jnp.int32(s), wait)


def _grad(name, work, block, h, dz, u, dy, into=None):
    V, T, D = h.shape
    F = dz.shape[-1]
    dma = pltpu.SemaphoreType.DMA
    pieces = 4
    args = [h, dz, u, dy] + list(into or ())
    return pl.pallas_call(
        functools.partial(_grads, work, block, pieces),
        out_shape=[jax.ShapeDtypeStruct((V, D, F), F32), jax.ShapeDtypeStruct((V, F, D), F32)],
        in_specs=[pl.BlockSpec(memory_space=pl.ANY)] * len(args),
        out_specs=[pl.BlockSpec(memory_space=pl.ANY)] * 2,
        scratch_shapes=[
            pltpu.VMEM((2, T, D), BF),
            pltpu.VMEM((2, T, block), BF),
            pltpu.VMEM((2, D, block), F32),
            pltpu.VMEM((2, block, D), F32),
            dma((2,)), dma((2,)), dma((2,)), dma((2 * pieces,)),
        ],
        input_output_aliases={4: 0, 5: 1} if into else {},
        compiler_params=pltpu.CompilerParams(vmem_limit_bytes=54 * 2 ** 20),
        cost_estimate=pl.CostEstimate(
            flops=2 * sum(w[3] for w in work) * T * D * block, bytes_accessed=sum(w[3] for w in work) * (2 * T * block + 4 * D * block), transcendentals=0),
        name=name,
    )(*args)


def _assemble(S, M, mine, other, far, back, y, dx, sem):
    p = lax.axis_index('stage')
    parity = lax.rem(p, 2)
    left = p < S // 2
    H = M // 2

    def put(src, k, dst, upper):
        pltpu.make_async_copy(src, dst.at[pl.ds(upper * H, H)], sem.at[k]).start()

    for k, src in enumerate((mine, other, far, back)):
        upper = parity if k % 2 == 0 else 1 - parity
        to_dx = left if k < 2 else jnp.logical_not(left)

        @pl.when(to_dx)
        def _():
            put(src, k, dx, upper)

        @pl.when(jnp.logical_not(to_dx))
        def _():
            put(src, k, y, upper)

    for k in range(4):
        pltpu.make_async_copy(mine, y.at[pl.ds(0, H)], sem.at[k]).wait()


def solution(mesh):
    S = mesh.shape['stage']

    def body(x, g, w1, w2):
        M, B, D = x.shape
        V, _, _, F = w1.shape
        w1 = w1[:, 0]
        w2 = w2[:, 0]
        G = GROUP
        n = V * M
        anys = pl.BlockSpec(memory_space=pl.ANY)
        dma = pltpu.SemaphoreType.DMA
        half = jax.ShapeDtypeStruct((M // 2, B, D), BF)
        u, dz, h, dy, mine, other = pl.pallas_call(
            functools.partial(_pipeline, S, V, M, G),
            out_shape=[
                jax.ShapeDtypeStruct((n, B, F), BF),
                jax.ShapeDtypeStruct((n, B, F), BF),
                jax.ShapeDtypeStruct((n, B, D), BF),
                jax.ShapeDtypeStruct((n, B, D), BF),
                half, half,
            ],
            in_specs=[anys] * 4,
            out_specs=[anys] * 6,
            scratch_shapes=[
                pltpu.VMEM((V, D, F), BF),
                pltpu.VMEM((V, F, D), BF),
                pltpu.VMEM((n + M, B, D), BF),
                pltpu.VMEM((n, B, D), BF),
                pltpu.VMEM((B, F), BF),
                pltpu.VMEM((2, B, F), BF),
                pltpu.VMEM((2, B, F), BF),
                pltpu.VMEM((2, B, D), BF),
                pltpu.VMEM((2, B, D), BF),
                dma((n + M,)), dma((n,)), dma((2,)), dma((2,)),
                dma((n,)), dma((n,)), dma((2,)), dma((2,)), dma((2 * V,)), dma((2,)), dma((M,)),
            ],
            compiler_params=pltpu.CompilerParams(
                collective_id=0, has_side_effects=True, vmem_limit_bytes=62 * 2 ** 20),
            cost_estimate=pl.CostEstimate(
                flops=10 * n * B * D * F, bytes_accessed=4 * n * B * F, transcendentals=3 * n * B * F),
            name='pipeline',
        )(x, g, w1, w2)

        h = h.reshape(V, M * B, D)
        dz = dz.reshape(V, M * B, F)
        u = u.reshape(V, M * B, F)
        dy = dy.reshape(V, M * B, D)

        far = lax.ppermute(mine, 'stage', [(q, (q + S // 2) % S) for q in range(S)])
        block = 1024 if F % 1024 == 0 else F // 3 if F % 384 == 0 else F // 2
        nb = F // block
        work = [(0, 0, 0, nb)] + [(1, v, 0, nb) for v in range(V)] + [(0, v, 0, nb) for v in range(1, V - 1)]
        d1, d2 = _grad('grads', work + [(0, V - 1, 0, nb - 2)] * (nb > 2), block, h, dz, u, dy)
        far, d1, d2 = lax.optimization_barrier((far, d1, d2))
        back = lax.ppermute(far, 'stage', [(q, q + 1 - 2 * (q % 2)) for q in range(S)])
        d1, d2 = _grad('grads_last', [(0, V - 1, nb - 2, 2)], block, h, dz, u, dy, (d1, d2))
        back, d1, d2 = lax.optimization_barrier((back, d1, d2))
        full = jax.ShapeDtypeStruct((M, B, D), BF)
        y, dx = pl.pallas_call(
            functools.partial(_assemble, S, M),
            out_shape=[full, full],
            in_specs=[pl.BlockSpec(memory_space=pltpu.VMEM)] * 4,
            out_specs=[anys] * 2,
            scratch_shapes=[dma((4,))],
            compiler_params=pltpu.CompilerParams(vmem_limit_bytes=16 * 2 ** 20),
            name='assemble',
        )(mine, other, far, back)
        return y, dx, d1[:, None], d2[:, None]

    act = P('data', None, None)
    wsp = P(None, 'stage', None, None)
    gsp = P('data', 'stage', None, None)
    return jax.shard_map(body, mesh=mesh, in_specs=(act, act, wsp, wsp), out_specs=(act, act, gsp, gsp), check_vma=False)
```

```python
import functools

import jax
import jax.numpy as jnp
from jax import lax
from jax.experimental import pallas as pl
from jax.experimental.pallas import tpu as pltpu
from jax.sharding import PartitionSpec as P

BF = jnp.bfloat16
F32 = jnp.float32
MESH = pl.DeviceIdType.MESH
NT = (((1,), (1,)), ((), ()))
GROUP = 8
ORDER = (
    'FFFFFFFFFFFFFFFFFFFFFBFMBBFBFBFBFBBFBFFBFBFBBBBBBBBBBBBBBBBBBBB',
    'FFFFFFFFFFFFFFFFFFBFFMBBBFBFBFBFBMFBFMFBFMBBBBBBBBBBBBBBBBBB',
    'FFFFFFFFFFFBFMFMMMMMMMMMMMBMMMMMMMBBBBBBBBBBB',
    'FFFFFFFFBFBMBBBMBFFBFBMBMFMMFFMMMMMBMMBBBBBBBBBFFFF',
)
WORD = 15


def _gelu(z):
    return 0.5 * z * (1.0 + lax.erf(z * 0.7071067811865476))


def _gelu_pair(z):
    half = 0.5 * (1.0 + lax.erf(z * 0.7071067811865476))
    return z * half, half + z * jnp.exp(-0.5 * z * z) * 0.3989422804014327


def _dot(a, b):
    return jnp.dot(a, b, preferred_element_type=F32)


def _dot_nt(a, b):
    return lax.dot_general(a, b, NT, preferred_element_type=F32)


def _words(row):
    return [sum('FBM'.index(c) * 4 ** b for b, c in enumerate(row[k:k + WORD])) for k in range(0, len(row), WORD)]


def _pipeline(S, V, M, G, x, g, w1_hbm, w2_hbm, u_out, dz_out, h_out, dy_out, mine, other,
              w1, w2, hbuf, dybuf, us, ub, dzb, fo, bo,
              f_recv, b_recv, f_send, b_send, h_sem, dy_sem, u_sem, dz_sem, w_sem, pair_send, pair_recv):
    p = lax.axis_index('stage')
    nxt = lax.rem(p + 1, S)
    prv = lax.rem(p + S - 1, S)
    parity = lax.rem(p, 2)
    partner = p + 1 - 2 * parity
    first = p == 0
    last = p == S - 1
    n = V * M
    H = M // 2
    F = w1.shape[-1]
    chunk = 256 if F % 256 == 0 else F

    barrier = pltpu.get_barrier_semaphore()
    for q in (prv, nxt):
        pl.semaphore_signal(barrier, inc=1, device_id={'stage': q}, device_id_type=MESH)

    def load_w(v):
        pltpu.make_async_copy(w1_hbm.at[v], w1.at[v], w_sem.at[2 * v]).start()
        pltpu.make_async_copy(w2_hbm.at[v], w2.at[v], w_sem.at[2 * v + 1]).start()

    def wait_w(v):
        pltpu.make_async_copy(w1_hbm.at[v], w1.at[v], w_sem.at[2 * v]).wait()
        pltpu.make_async_copy(w2_hbm.at[v], w2.at[v], w_sem.at[2 * v + 1]).wait()

    def load_x(m):
        pltpu.make_async_copy(x.at[m], hbuf.at[m], f_recv.at[m]).start()

    def load_g(m):
        s = (V - 1) * M + m
        pltpu.make_async_copy(g.at[m], dybuf.at[s], b_recv.at[s]).start()

    @pl.when(first)
    def _():
        load_x(0)

    load_w(0)

    @pl.when(first)
    def _():
        lax.fori_loop(1, M, lambda m, c: (load_x(m), c)[1], 0)

    for v in range(1, V):
        load_w(v)

    @pl.when(last)
    def _():
        lax.fori_loop(0, M, lambda m, c: (load_g(m), c)[1], 0)

    pl.semaphore_wait(barrier, 2)
    wait_w(0)

    def place(i):
        blk, r = i // (V * G), lax.rem(i, V * G)
        return r // G, blk * G + lax.rem(r, G)

    def place_f(i):
        v, m = place(i)
        early = i < G + G // 2
        v = jnp.where(last, jnp.where(i < G, 0, jnp.where(early, 1, jnp.where(i < 2 * G + G // 2, 0, 1))), v)
        m = jnp.where(last, jnp.where(i < G, i, jnp.where(early, i - G, jnp.where(i < 2 * G + G // 2, i - G // 2, i - 2 * G))), m)
        return v, m

    def wait_f_send(i):
        s = lax.rem(i, 2)
        pltpu.make_async_copy(fo.at[s], mine.at[0], f_send.at[s]).wait()

        @pl.when(last & (place_f(i)[0] == V - 1))
        def _():
            pltpu.make_async_copy(fo.at[s], mine.at[0], pair_send.at[s]).wait()

    def wait_b_send(j):
        s = lax.rem(j, 2)
        pltpu.make_async_copy(bo.at[s], mine.at[0], b_send.at[s]).wait()

        @pl.when(first & (place(j)[0] == V - 1))
        def _():
            pltpu.make_async_copy(bo.at[s], mine.at[0], pair_send.at[s]).wait()

    def wait_uz(s):
        pltpu.make_async_copy(ub.at[s], u_out.at[0], u_sem.at[s]).wait()
        pltpu.make_async_copy(dzb.at[s], dz_out.at[0], dz_sem.at[s]).wait()

    def take_h(slot):
        pltpu.make_async_copy(fo.at[0], hbuf.at[slot], f_recv.at[slot]).wait()
        pltpu.make_async_copy(hbuf.at[slot], h_out.at[slot], h_sem.at[slot]).start()

    def halves(m, put):
        own = m // H == parity

        @pl.when(own)
        def _():
            put(mine, other)

        @pl.when(jnp.logical_not(own))
        def _():
            put(other, mine)

    def ready_f(i):
        v, m = place_f(i)

        @pl.when(i == G - 1)
        def _():
            for vv in range(1, V):
                wait_w(vv)

        @pl.when(jnp.logical_not(last & (v == V - 1)))
        def _():
            take_h(v * M + m)

        @pl.when(i >= 2)
        def _():
            wait_f_send(i - 2)

    def compute_f(i):
        v, m = place_f(i)
        slot = v * M + m
        s = lax.rem(i, 2)
        for c in range(F // chunk):
            cs = slice(c * chunk, (c + 1) * chunk)
            us[:, cs] = _gelu(_dot(hbuf[slot], w1[v, :, cs])).astype(BF)
        fo[s] = (hbuf[slot].astype(F32) + _dot(us[...], w2[v])).astype(BF)

    def done_f(i):
        v, m = place_f(i)
        slot = v * M + m
        s = lax.rem(i, 2)
        final = last & (v == V - 1)

        @pl.when(final)
        def _():
            k = lax.rem(m, H)

            def put(here, there):
                pltpu.make_async_copy(fo.at[s], here.at[k], f_send.at[s]).start()
                pltpu.make_async_remote_copy(
                    src_ref=fo.at[s], dst_ref=there.at[k], send_sem=pair_send.at[s], recv_sem=pair_recv.at[m],
                    device_id={'stage': partner}, device_id_type=MESH).start()

            halves(m, put)

        @pl.when(jnp.logical_not(final))
        def _():
            to = slot + jnp.where(last, M, 0)
            pltpu.make_async_remote_copy(
                src_ref=fo.at[s], dst_ref=hbuf.at[to], send_sem=f_send.at[s], recv_sem=f_recv.at[to],
                device_id={'stage': nxt}, device_id_type=MESH).start()

    def place_b(j):
        vr, m = place(j)
        return V - 1 - vr, m

    def ready_b(j):
        v, m = place_b(j)
        slot = v * M + m

        @pl.when(last & (v == V - 1))
        def _():
            take_h(slot)

        pltpu.make_async_copy(bo.at[0], dybuf.at[slot], b_recv.at[slot]).wait()
        pltpu.make_async_copy(dybuf.at[slot], dy_out.at[slot], dy_sem.at[slot]).start()

        @pl.when(j >= 2)
        def _():
            wait_b_send(j - 2)
            wait_uz(lax.rem(j, 2))

    def compute_b(j):
        v, m = place_b(j)
        slot = v * M + m
        s = lax.rem(j, 2)
        for c in range(F // chunk):
            cs = slice(c * chunk, (c + 1) * chunk)
            a, b = _gelu_pair(_dot(hbuf[slot], w1[v, :, cs]))
            ub[s, :, cs] = a.astype(BF)
            dzb[s, :, cs] = (_dot_nt(dybuf[slot], w2[v, cs, :]) * b).astype(BF)
        pltpu.make_async_copy(ub.at[s], u_out.at[slot], u_sem.at[s]).start()
        bo[s] = (dybuf[slot].astype(F32) + _dot_nt(dzb[s], w1[v])).astype(BF)

    def done_b(j):
        v, m = place_b(j)
        slot = v * M + m
        s = lax.rem(j, 2)
        final = first & (v == 0)
        to = jnp.where(final, n + m, slot - jnp.where(first, M, 0))
        pltpu.make_async_remote_copy(
            src_ref=bo.at[s], dst_ref=dybuf.at[to], send_sem=b_send.at[s], recv_sem=b_recv.at[to],
            device_id={'stage': jnp.where(final, partner, prv)}, device_id_type=MESH).start()
        pltpu.make_async_copy(dzb.at[s], dz_out.at[slot], dz_sem.at[s]).start()

        @pl.when(final)
        def _():
            halves(m, lambda here, there: pltpu.make_async_copy(
                bo.at[s], here.at[lax.rem(m, H)], pair_send.at[s]).start())

    table = [_words(row) for row in ORDER]

    def word(k):
        out = jnp.int32(0)
        for q in range(S):
            for b in range(len(table[q])):
                out = jnp.where((p == q) & (k == b), table[q][b], out)
        return out

    def step(t, carry):
        i, j, bits = carry
        bits = jnp.where(lax.rem(t, WORD) == 0, word(t // WORD), bits)
        kind = lax.rem(bits, 4)

        @pl.when(kind == 0)
        def _():
            ready_f(i)
            compute_f(i)
            done_f(i)

        @pl.when(kind == 1)
        def _():
            ready_b(j)
            compute_b(j)
            done_b(j)

        @pl.when(kind == 2)
        def _():
            ready_b(j)
            ready_f(i)
            compute_b(j)
            compute_f(i)
            done_b(j)
            done_f(i)

        return i + jnp.where(kind == 1, 0, 1), j + jnp.where(kind == 0, 0, 1), bits // 4

    zero = jnp.int32(0)
    count = jnp.int32(0)
    for q in range(S):
        count = jnp.where(p == q, len(ORDER[q]), count)
    lax.fori_loop(0, count, step, (zero, zero, zero))

    for k in (n - 2, n - 1):
        wait_f_send(jnp.int32(k))
        wait_b_send(jnp.int32(k))
        wait_uz(k % 2)

    @pl.when(p == 1)
    def _():
        def take(m, c):
            pltpu.make_async_copy(bo.at[0], dybuf.at[n + m], b_recv.at[n + m]).wait()
            return c

        lax.fori_loop(0, M, take, 0)
        copies = [pltpu.make_async_copy(dybuf.at[pl.ds(n + k * H, H)], ref, pair_send.at[k]) for k, ref in enumerate((other, mine))]
        for c in copies:
            c.start()
        for c in copies:
            c.wait()

    def drain(slot, carry):
        pltpu.make_async_copy(hbuf.at[slot], h_out.at[slot], h_sem.at[slot]).wait()
        pltpu.make_async_copy(dybuf.at[slot], dy_out.at[slot], dy_sem.at[slot]).wait()
        return carry

    lax.fori_loop(0, n, drain, 0)

    @pl.when(p == S - 2)
    def _():
        lax.fori_loop(
            0, M, lambda m, c: (pltpu.make_async_copy(fo.at[0], mine.at[0], pair_recv.at[m]).wait(), c)[1], 0)


def _grads(work, block, pieces, S, spread, h, dz, u, dy, *rest):
    if spread:
        parts = rest[2:5]
        d1, d2, y, dx, narrow, wide, o1, o2, n_sem, w_sem, o_sem, p_sem, stage, s_sem = rest[-14:]
        loads = [pltpu.make_async_copy(ref, stage.at[k], s_sem.at[k]) for k, ref in enumerate(parts)]
    else:
        d1, d2, narrow, wide, o1, o2, n_sem, w_sem, o_sem, p_sem = rest[-10:]
    T = wide.shape[1]
    begin = [sum(w[3] for w in work[:q]) for q in range(len(work) + 1)]
    total = begin[-1]
    tn = (((0,), (0,)), ((), ()))
    kinds = [w[0] for w in work]

    def pick(s, values):
        out = jnp.int32(values[0])
        for q in range(1, len(work)):
            out = jnp.where(s >= begin[q], values[q], out)
        return out

    def at(s):
        v = pick(s, [w[1] for w in work])
        blk = s + pick(s, [w[2] - begin[q] for q, w in enumerate(work)])
        return pick(s, kinds), v, pl.ds(pl.multiple_of(blk * block, block), block), lax.rem(s, 2)

    def narrow_copy(q, act):
        act(pltpu.make_async_copy((dy if kinds[q] else h).at[work[q][1]], narrow.at[q % 2], n_sem.at[q % 2]))

    def wide_copy(s, act):
        kind, v, cols, slot = at(s)
        for k, src in ((0, dz), (1, u)):
            if k in kinds:
                @pl.when(kind == k)
                def _():
                    act(pltpu.make_async_copy(src.at[v, :, cols], wide.at[slot], w_sem.at[slot]))

    def out_copy(s, act):
        kind, v, cols, slot = at(s)
        if 0 in kinds:
            @pl.when(kind == 0)
            def _():
                act(pltpu.make_async_copy(o1.at[slot], d1.at[v, :, cols], o_sem.at[slot]))
        if 1 in kinds:
            @pl.when(kind == 1)
            def _():
                act(pltpu.make_async_copy(o2.at[slot], d2.at[v, cols, :], o_sem.at[slot]))

    start = lambda c: c.start()
    wait = lambda c: c.wait()
    rows = T // pieces

    def piece(r, act):
        sl = pl.ds(pl.multiple_of(r * rows, rows), rows)
        act(pltpu.make_async_copy(h.at[work[0][1], sl], narrow.at[0, sl], p_sem.at[2 * r]))
        act(pltpu.make_async_copy(dz.at[work[0][1], sl, pl.ds(work[0][2] * block, block)], wide.at[0, sl], p_sem.at[2 * r + 1]))

    for r in range(pieces):
        piece(r, start)
    wide_copy(jnp.int32(1), start)
    if len(work) > 1:
        narrow_copy(1, start)
    if spread:
        for c in loads:
            c.start()

    piece(0, wait)
    o1[0] = lax.dot_general(narrow[0, :rows], wide[0, :rows], tn, preferred_element_type=F32)

    def add(r, carry):
        piece(r, wait)
        sl = pl.ds(pl.multiple_of(r * rows, rows), rows)
        o1[0] += lax.dot_general(narrow[0, sl], wide[0, sl], tn, preferred_element_type=F32)
        return carry

    lax.fori_loop(1, pieces, add, jnp.int32(0))
    out_copy(jnp.int32(0), start)
    if spread:
        for c in loads:
            c.wait()
        _spread(S, [stage.at[k] for k in range(len(parts))], y, dx, s_sem)

    def step(s, carry):
        kind, _, _, slot = at(s)
        side = pick(s, [q % 2 for q in range(len(work))])
        wide_copy(s, wait)
        for q in range(1, len(work)):
            @pl.when(s == begin[q])
            def _():
                narrow_copy(q, wait)
                if q + 1 < len(work):
                    narrow_copy(q + 1, start)

        @pl.when(s + 1 < total)
        def _():
            wide_copy(s + 1, start)

        @pl.when(s >= 2)
        def _():
            out_copy(s - 2, wait)

        if 0 in kinds:
            @pl.when(kind == 0)
            def _():
                o1[slot] = lax.dot_general(narrow[side], wide[slot], tn, preferred_element_type=F32)
        if 1 in kinds:
            @pl.when(kind == 1)
            def _():
                o2[slot] = lax.dot_general(wide[slot], narrow[side], tn, preferred_element_type=F32)
        out_copy(s, start)
        return carry

    lax.fori_loop(1, total, step, jnp.int32(0))
    for s in (total - 2, total - 1):
        out_copy(jnp.int32(s), wait)
    if spread:
        for k in range(len(parts)):
            pltpu.make_async_copy(stage.at[k], y.at[pl.ds(0, stage.shape[1])], s_sem.at[k]).wait()


def _grad(name, work, block, S, h, dz, u, dy, into=None, parts=None):
    V, T, D = h.shape
    F = dz.shape[-1]
    dma = pltpu.SemaphoreType.DMA
    pieces = 4
    hbm = pl.BlockSpec(memory_space=pltpu.HBM)
    kinds = [w[0] for w in work]
    args = [h, dz, u, dy] + list(into or ()) + list(parts or ())
    outs = [jax.ShapeDtypeStruct((V, D, F), F32), jax.ShapeDtypeStruct((V, F, D), F32)]
    scratch = [
        pltpu.VMEM((2 if len(work) > 1 else 1, T, D), BF),
        pltpu.VMEM((2, T, block), BF),
        pltpu.VMEM((2, D, block), F32),
        pltpu.VMEM((2, block, D) if 1 in kinds else (8, 128), F32),
        dma((2,)), dma((2,)), dma((2,)), dma((2 * pieces,)),
    ]
    if parts:
        H, B, _ = parts[0].shape
        outs += [jax.ShapeDtypeStruct((2 * H, B, D), BF)] * 2
        scratch += [pltpu.VMEM((len(parts), H, B, D), BF), dma((len(parts),))]
    return pl.pallas_call(
        functools.partial(_grads, work, block, pieces, S, bool(parts)),
        out_shape=outs,
        in_specs=[hbm] * len(args),
        out_specs=[hbm] * len(outs),
        scratch_shapes=scratch,
        input_output_aliases={4: 0, 5: 1} if into else {},
        compiler_params=pltpu.CompilerParams(vmem_limit_bytes=54 * 2 ** 20),
        cost_estimate=pl.CostEstimate(
            flops=2 * sum(w[3] for w in work) * T * D * block, bytes_accessed=sum(w[3] for w in work) * (2 * T * block + 4 * D * block), transcendentals=0),
        name=name,
    )(*args)


def _spread(S, parts, y, dx, sem, begin=0):
    p = lax.axis_index('stage')
    parity = lax.rem(p, 2)
    left = p < S // 2
    for k, src in enumerate(parts):
        H = src.shape[0]
        upper = parity if (begin + k) % 2 == 0 else 1 - parity
        to_dx = left if begin + k < 2 else jnp.logical_not(left)
        rows = pl.ds(upper * H, H)

        @pl.when(to_dx)
        def _():
            pltpu.make_async_copy(src, dx.at[rows], sem.at[k]).start()

        @pl.when(jnp.logical_not(to_dx))
        def _():
            pltpu.make_async_copy(src, y.at[rows], sem.at[k]).start()


def _finish(S, back, y_in, dx_in, y, dx, sem):
    _spread(S, [back], y, dx, sem, 3)
    pltpu.make_async_copy(back, y.at[pl.ds(0, back.shape[0])], sem.at[0]).wait()


def solution(mesh):
    S = mesh.shape['stage']

    def body(x, g, w1, w2):
        M, B, D = x.shape
        V, _, _, F = w1.shape
        w1 = w1[:, 0]
        w2 = w2[:, 0]
        G = GROUP
        n = V * M
        anys = pl.BlockSpec(memory_space=pl.ANY)
        dma = pltpu.SemaphoreType.DMA
        half = jax.ShapeDtypeStruct((M // 2, B, D), BF)
        u, dz, h, dy, mine, other = pl.pallas_call(
            functools.partial(_pipeline, S, V, M, G),
            out_shape=[
                jax.ShapeDtypeStruct((n, B, F), BF),
                jax.ShapeDtypeStruct((n, B, F), BF),
                jax.ShapeDtypeStruct((n, B, D), BF),
                jax.ShapeDtypeStruct((n, B, D), BF),
                half, half,
            ],
            in_specs=[anys] * 4,
            out_specs=[anys] * 6,
            scratch_shapes=[
                pltpu.VMEM((V, D, F), BF),
                pltpu.VMEM((V, F, D), BF),
                pltpu.VMEM((n, B, D), BF),
                pltpu.VMEM((n + M, B, D), BF),
                pltpu.VMEM((B, F), BF),
                pltpu.VMEM((2, B, F), BF),
                pltpu.VMEM((2, B, F), BF),
                pltpu.VMEM((2, B, D), BF),
                pltpu.VMEM((2, B, D), BF),
                dma((n,)), dma((n + M,)), dma((2,)), dma((2,)),
                dma((n,)), dma((n,)), dma((2,)), dma((2,)), dma((2 * V,)), dma((2,)), dma((M,)),
            ],
            compiler_params=pltpu.CompilerParams(
                collective_id=0, has_side_effects=True, vmem_limit_bytes=62 * 2 ** 20),
            cost_estimate=pl.CostEstimate(
                flops=10 * n * B * D * F, bytes_accessed=4 * n * B * F, transcendentals=3 * n * B * F),
            name='pipeline',
        )(x, g, w1, w2)

        h = h.reshape(V, M * B, D)
        dz = dz.reshape(V, M * B, F)
        u = u.reshape(V, M * B, F)
        dy = dy.reshape(V, M * B, D)

        far = lax.ppermute(mine, 'stage', [(q, (q + S // 2) % S) for q in range(S)])
        block = 1024 if F % 1024 == 0 else F // 3 if F % 384 == 0 else F // 2
        nb = F // block
        work = [(0, 0, 0, nb)] + [(1, v, 0, nb) for v in range(V)] + [(0, v, 0, nb) for v in range(1, V - 1)]
        d1, d2 = _grad('grads', work + [(0, V - 1, 0, nb - 2)] * (nb > 2), block, S, h, dz, u, dy)
        far, d1, d2 = lax.optimization_barrier((far, d1, d2))
        back = lax.ppermute(far, 'stage', [(q, q + 1 - 2 * (q % 2)) for q in range(S)])
        d1, d2, y, dx = _grad(
            'grads_last', [(0, V - 1, nb - 2, 2)], block, S, h, dz, u, dy, (d1, d2), (mine, other, far))
        back, d1, d2, y, dx = lax.optimization_barrier((back, d1, d2, y, dx))
        full = jax.ShapeDtypeStruct((M, B, D), BF)
        hbm = pl.BlockSpec(memory_space=pltpu.HBM)
        y, dx = pl.pallas_call(
            functools.partial(_finish, S),
            out_shape=[full, full],
            in_specs=[pl.BlockSpec(memory_space=pltpu.VMEM), hbm, hbm],
            out_specs=[hbm, hbm],
            scratch_shapes=[dma((1,))],
            input_output_aliases={1: 0, 2: 1},
            compiler_params=pltpu.CompilerParams(vmem_limit_bytes=16 * 2 ** 20),
            name='last_quarter',
        )(back, y, dx)
        return y, dx, d1[:, None], d2[:, None]

    act = P('data', None, None)
    wsp = P(None, 'stage', None, None)
    gsp = P('data', 'stage', None, None)
    return jax.shard_map(body, mesh=mesh, in_specs=(act, act, wsp, wsp), out_specs=(act, act, gsp, gsp), check_vma=False)
```

```python
import functools

import jax
import jax.numpy as jnp
from jax import lax
from jax.experimental import pallas as pl
from jax.experimental.pallas import tpu as pltpu
from jax.sharding import PartitionSpec as P

BF = jnp.bfloat16
F32 = jnp.float32
MESH = pl.DeviceIdType.MESH
NT = (((1,), (1,)), ((), ()))
GROUP = 8
ORDER = (
    'FFFFFFFFFFFFFFFFFFFFBFBFBFBBFBBFFBBFFFBBFFBFBBBBBBBBBBBBBBBBBBBB',
    'FFFFFFFFFFFFFFFFFBFBBFFFFBBBFFBBBFBFFFBFBFBFBFBBBBBBBBBBBBBBBBBB',
    'FFFFFFFFFFFBBFFBFBFFBBBBBFFFBFFFBBFFBBFBFBFBFFFBBFBBFBBBBBBBBBBB',
    'FFFFFFFFBBFFBBBFBBBBFBBFFFBFBFBFFBFFBFBBFBFBFFBBFBBBBBBBBBBFFFFF',
)
WORD = 16


def _gelu(z):
    return 0.5 * z * (1.0 + lax.erf(z * 0.7071067811865476))


def _gelu_pair(z):
    half = 0.5 * (1.0 + lax.erf(z * 0.7071067811865476))
    return z * half, half + z * jnp.exp(-0.5 * z * z) * 0.3989422804014327


def _dot(a, b):
    return jnp.dot(a, b, preferred_element_type=F32)


def _dot_nt(a, b):
    return lax.dot_general(a, b, NT, preferred_element_type=F32)


def _words(row):
    return [sum('FB'.index(c) * 2 ** b for b, c in enumerate(row[k:k + WORD])) for k in range(0, len(row), WORD)]


def _pipeline(S, V, M, G, x, g, w1_hbm, w2_hbm, u_out, dz_out, h_out, dy_out, mine, other,
              w1, w2, hbuf, dybuf, us, ub, dzb, fo, bo,
              f_recv, b_recv, f_send, b_send, h_sem, dy_sem, u_sem, dz_sem, w_sem, pair_send, pair_recv):
    p = lax.axis_index('stage')
    nxt = lax.rem(p + 1, S)
    prv = lax.rem(p + S - 1, S)
    parity = lax.rem(p, 2)
    partner = p + 1 - 2 * parity
    first = p == 0
    last = p == S - 1
    n = V * M
    H = M // 2
    F = w1.shape[-1]
    chunk = 256 if F % 256 == 0 else F

    barrier = pltpu.get_barrier_semaphore()
    for q in (prv, nxt):
        pl.semaphore_signal(barrier, inc=1, device_id={'stage': q}, device_id_type=MESH)

    def load_w(v):
        pltpu.make_async_copy(w1_hbm.at[v], w1.at[v], w_sem.at[2 * v]).start()
        pltpu.make_async_copy(w2_hbm.at[v], w2.at[v], w_sem.at[2 * v + 1]).start()

    def wait_w(v):
        pltpu.make_async_copy(w1_hbm.at[v], w1.at[v], w_sem.at[2 * v]).wait()
        pltpu.make_async_copy(w2_hbm.at[v], w2.at[v], w_sem.at[2 * v + 1]).wait()

    def load_x(m):
        pltpu.make_async_copy(x.at[m], hbuf.at[m], f_recv.at[m]).start()

    def load_g(m):
        s = (V - 1) * M + m
        pltpu.make_async_copy(g.at[m], dybuf.at[s], b_recv.at[s]).start()

    @pl.when(first)
    def _():
        load_x(0)

    load_w(0)

    @pl.when(first)
    def _():
        lax.fori_loop(1, M, lambda m, c: (load_x(m), c)[1], 0)

    for v in range(1, V):
        load_w(v)

    @pl.when(last)
    def _():
        lax.fori_loop(0, M, lambda m, c: (load_g(m), c)[1], 0)

    pl.semaphore_wait(barrier, 2)
    wait_w(0)

    def place(i):
        blk, r = i // (V * G), lax.rem(i, V * G)
        return r // G, blk * G + lax.rem(r, G)

    def place_f(i):
        v, m = place(i)
        early = i < G + G // 2
        v = jnp.where(last, jnp.where(i < G, 0, jnp.where(early, 1, jnp.where(i < 2 * G + G // 2, 0, 1))), v)
        m = jnp.where(last, jnp.where(i < G, i, jnp.where(early, i - G, jnp.where(i < 2 * G + G // 2, i - G // 2, i - 2 * G))), m)
        return v, m

    def wait_f_send(i):
        s = lax.rem(i, 2)
        pltpu.make_async_copy(fo.at[s], mine.at[0], f_send.at[s]).wait()

        @pl.when(last & (place_f(i)[0] == V - 1))
        def _():
            pltpu.make_async_copy(fo.at[s], mine.at[0], pair_send.at[s]).wait()

    def wait_b_send(j):
        s = lax.rem(j, 2)
        pltpu.make_async_copy(bo.at[s], mine.at[0], b_send.at[s]).wait()

        @pl.when(first & (place(j)[0] == V - 1))
        def _():
            pltpu.make_async_copy(bo.at[s], mine.at[0], pair_send.at[s]).wait()

    def wait_uz(s):
        pltpu.make_async_copy(ub.at[s], u_out.at[0], u_sem.at[s]).wait()
        pltpu.make_async_copy(dzb.at[s], dz_out.at[0], dz_sem.at[s]).wait()

    def take_h(slot):
        pltpu.make_async_copy(fo.at[0], hbuf.at[slot], f_recv.at[slot]).wait()
        pltpu.make_async_copy(hbuf.at[slot], h_out.at[slot], h_sem.at[slot]).start()

    def halves(m, put):
        own = m // H == parity

        @pl.when(own)
        def _():
            put(mine, other)

        @pl.when(jnp.logical_not(own))
        def _():
            put(other, mine)

    def ready_f(i):
        v, m = place_f(i)

        @pl.when(i == G - 1)
        def _():
            for vv in range(1, V):
                wait_w(vv)

        @pl.when(jnp.logical_not(last & (v == V - 1)))
        def _():
            take_h(v * M + m)

        @pl.when(i >= 2)
        def _():
            wait_f_send(i - 2)

    def compute_f(i):
        v, m = place_f(i)
        slot = v * M + m
        s = lax.rem(i, 2)
        for c in range(F // chunk):
            cs = slice(c * chunk, (c + 1) * chunk)
            us[:, cs] = _gelu(_dot(hbuf[slot], w1[v, :, cs])).astype(BF)
        fo[s] = (hbuf[slot].astype(F32) + _dot(us[...], w2[v])).astype(BF)

    def done_f(i):
        v, m = place_f(i)
        slot = v * M + m
        s = lax.rem(i, 2)
        final = last & (v == V - 1)

        @pl.when(final)
        def _():
            k = lax.rem(m, H)

            def put(here, there):
                pltpu.make_async_copy(fo.at[s], here.at[k], f_send.at[s]).start()
                pltpu.make_async_remote_copy(
                    src_ref=fo.at[s], dst_ref=there.at[k], send_sem=pair_send.at[s], recv_sem=pair_recv.at[m],
                    device_id={'stage': partner}, device_id_type=MESH).start()

            halves(m, put)

        @pl.when(jnp.logical_not(final))
        def _():
            to = slot + jnp.where(last, M, 0)
            pltpu.make_async_remote_copy(
                src_ref=fo.at[s], dst_ref=hbuf.at[to], send_sem=f_send.at[s], recv_sem=f_recv.at[to],
                device_id={'stage': nxt}, device_id_type=MESH).start()

    def place_b(j):
        vr, m = place(j)
        return V - 1 - vr, m

    def ready_b(j):
        v, m = place_b(j)
        slot = v * M + m

        @pl.when(last & (v == V - 1))
        def _():
            take_h(slot)

        pltpu.make_async_copy(bo.at[0], dybuf.at[slot], b_recv.at[slot]).wait()
        pltpu.make_async_copy(dybuf.at[slot], dy_out.at[slot], dy_sem.at[slot]).start()

        @pl.when(j >= 2)
        def _():
            wait_b_send(j - 2)
            wait_uz(lax.rem(j, 2))

    def compute_b(j):
        v, m = place_b(j)
        slot = v * M + m
        s = lax.rem(j, 2)
        for c in range(F // chunk):
            cs = slice(c * chunk, (c + 1) * chunk)
            a, b = _gelu_pair(_dot(hbuf[slot], w1[v, :, cs]))
            ub[s, :, cs] = a.astype(BF)
            dzb[s, :, cs] = (_dot_nt(dybuf[slot], w2[v, cs, :]) * b).astype(BF)
        pltpu.make_async_copy(ub.at[s], u_out.at[slot], u_sem.at[s]).start()
        bo[s] = (dybuf[slot].astype(F32) + _dot_nt(dzb[s], w1[v])).astype(BF)

    def done_b(j):
        v, m = place_b(j)
        slot = v * M + m
        s = lax.rem(j, 2)
        final = first & (v == 0)
        to = jnp.where(final, n + m, slot - jnp.where(first, M, 0))
        pltpu.make_async_remote_copy(
            src_ref=bo.at[s], dst_ref=dybuf.at[to], send_sem=b_send.at[s], recv_sem=b_recv.at[to],
            device_id={'stage': jnp.where(final, partner, prv)}, device_id_type=MESH).start()
        pltpu.make_async_copy(dzb.at[s], dz_out.at[slot], dz_sem.at[s]).start()

        @pl.when(final)
        def _():
            halves(m, lambda here, there: pltpu.make_async_copy(
                bo.at[s], here.at[lax.rem(m, H)], pair_send.at[s]).start())

    table = [_words(row) for row in ORDER]

    def word(k):
        out = jnp.int32(0)
        for q in range(S):
            for b in range(len(table[q])):
                out = jnp.where((p == q) & (k == b), table[q][b], out)
        return out

    def step(t, carry):
        i, j, bits = carry
        bits = jnp.where(lax.rem(t, WORD) == 0, word(t // WORD), bits)
        kind = lax.rem(bits, 2)

        @pl.when(kind == 0)
        def _():
            ready_f(i)
            compute_f(i)
            done_f(i)

        @pl.when(kind == 1)
        def _():
            ready_b(j)
            compute_b(j)
            done_b(j)

        return i + 1 - kind, j + kind, bits // 2

    zero = jnp.int32(0)
    lax.fori_loop(0, 2 * n, step, (zero, zero, zero))

    for k in (n - 2, n - 1):
        wait_f_send(jnp.int32(k))
        wait_b_send(jnp.int32(k))
        wait_uz(k % 2)

    @pl.when(p == 1)
    def _():
        def take(m, c):
            pltpu.make_async_copy(bo.at[0], dybuf.at[n + m], b_recv.at[n + m]).wait()
            return c

        lax.fori_loop(0, M, take, 0)
        copies = [pltpu.make_async_copy(dybuf.at[pl.ds(n + k * H, H)], ref, pair_send.at[k]) for k, ref in enumerate((other, mine))]
        for c in copies:
            c.start()
        for c in copies:
            c.wait()

    def drain(slot, carry):
        pltpu.make_async_copy(hbuf.at[slot], h_out.at[slot], h_sem.at[slot]).wait()
        pltpu.make_async_copy(dybuf.at[slot], dy_out.at[slot], dy_sem.at[slot]).wait()
        return carry

    lax.fori_loop(0, n, drain, 0)

    @pl.when(p == S - 2)
    def _():
        lax.fori_loop(
            0, M, lambda m, c: (pltpu.make_async_copy(fo.at[0], mine.at[0], pair_recv.at[m]).wait(), c)[1], 0)


def _grads(work, block, pieces, S, spread, h, dz, u, dy, *rest):
    if spread:
        parts = rest[2:5]
        d1, d2, y, dx, narrow, wide, o1, o2, n_sem, w_sem, o_sem, p_sem, stage, s_sem = rest[-14:]
        loads = [pltpu.make_async_copy(ref, stage.at[k], s_sem.at[k]) for k, ref in enumerate(parts)]
    else:
        d1, d2, narrow, wide, o1, o2, n_sem, w_sem, o_sem, p_sem = rest[-10:]
    T = wide.shape[1]
    begin = [sum(w[3] for w in work[:q]) for q in range(len(work) + 1)]
    total = begin[-1]
    tn = (((0,), (0,)), ((), ()))
    kinds = [w[0] for w in work]

    def pick(s, values):
        out = jnp.int32(values[0])
        for q in range(1, len(work)):
            out = jnp.where(s >= begin[q], values[q], out)
        return out

    def at(s):
        v = pick(s, [w[1] for w in work])
        blk = s + pick(s, [w[2] - begin[q] for q, w in enumerate(work)])
        return pick(s, kinds), v, pl.ds(pl.multiple_of(blk * block, block), block), lax.rem(s, 2)

    def narrow_copy(q, act):
        act(pltpu.make_async_copy((dy if kinds[q] else h).at[work[q][1]], narrow.at[q % 2], n_sem.at[q % 2]))

    def wide_copy(s, act):
        kind, v, cols, slot = at(s)
        for k, src in ((0, dz), (1, u)):
            if k in kinds:
                @pl.when(kind == k)
                def _():
                    act(pltpu.make_async_copy(src.at[v, :, cols], wide.at[slot], w_sem.at[slot]))

    def out_copy(s, act):
        kind, v, cols, slot = at(s)
        if 0 in kinds:
            @pl.when(kind == 0)
            def _():
                act(pltpu.make_async_copy(o1.at[slot], d1.at[v, :, cols], o_sem.at[slot]))
        if 1 in kinds:
            @pl.when(kind == 1)
            def _():
                act(pltpu.make_async_copy(o2.at[slot], d2.at[v, cols, :], o_sem.at[slot]))

    start = lambda c: c.start()
    wait = lambda c: c.wait()
    rows = T // pieces

    def piece(r, act):
        sl = pl.ds(pl.multiple_of(r * rows, rows), rows)
        act(pltpu.make_async_copy(h.at[work[0][1], sl], narrow.at[0, sl], p_sem.at[2 * r]))
        act(pltpu.make_async_copy(dz.at[work[0][1], sl, pl.ds(work[0][2] * block, block)], wide.at[0, sl], p_sem.at[2 * r + 1]))

    for r in range(pieces):
        piece(r, start)
    wide_copy(jnp.int32(1), start)
    if len(work) > 1:
        narrow_copy(1, start)
    if spread:
        for c in loads:
            c.start()

    piece(0, wait)
    o1[0] = lax.dot_general(narrow[0, :rows], wide[0, :rows], tn, preferred_element_type=F32)

    def add(r, carry):
        piece(r, wait)
        sl = pl.ds(pl.multiple_of(r * rows, rows), rows)
        o1[0] += lax.dot_general(narrow[0, sl], wide[0, sl], tn, preferred_element_type=F32)
        return carry

    lax.fori_loop(1, pieces, add, jnp.int32(0))
    out_copy(jnp.int32(0), start)
    if spread:
        for c in loads:
            c.wait()
        _spread(S, [stage.at[k] for k in range(len(parts))], y, dx, s_sem)

    def step(s, carry):
        kind, _, _, slot = at(s)
        side = pick(s, [q % 2 for q in range(len(work))])
        wide_copy(s, wait)
        for q in range(1, len(work)):
            @pl.when(s == begin[q])
            def _():
                narrow_copy(q, wait)
                if q + 1 < len(work):
                    narrow_copy(q + 1, start)

        @pl.when(s + 1 < total)
        def _():
            wide_copy(s + 1, start)

        @pl.when(s >= 2)
        def _():
            out_copy(s - 2, wait)

        if 0 in kinds:
            @pl.when(kind == 0)
            def _():
                o1[slot] = lax.dot_general(narrow[side], wide[slot], tn, preferred_element_type=F32)
        if 1 in kinds:
            @pl.when(kind == 1)
            def _():
                o2[slot] = lax.dot_general(wide[slot], narrow[side], tn, preferred_element_type=F32)
        out_copy(s, start)
        return carry

    lax.fori_loop(1, total, step, jnp.int32(0))
    for s in (total - 2, total - 1):
        out_copy(jnp.int32(s), wait)
    if spread:
        for k in range(len(parts)):
            pltpu.make_async_copy(stage.at[k], y.at[pl.ds(0, stage.shape[1])], s_sem.at[k]).wait()


def _grad(name, work, block, S, h, dz, u, dy, into=None, parts=None):
    V, T, D = h.shape
    F = dz.shape[-1]
    dma = pltpu.SemaphoreType.DMA
    pieces = 4
    hbm = pl.BlockSpec(memory_space=pltpu.HBM)
    kinds = [w[0] for w in work]
    args = [h, dz, u, dy] + list(into or ()) + list(parts or ())
    outs = [jax.ShapeDtypeStruct((V, D, F), F32), jax.ShapeDtypeStruct((V, F, D), F32)]
    scratch = [
        pltpu.VMEM((2 if len(work) > 1 else 1, T, D), BF),
        pltpu.VMEM((2, T, block), BF),
        pltpu.VMEM((2, D, block), F32),
        pltpu.VMEM((2, block, D) if 1 in kinds else (8, 128), F32),
        dma((2,)), dma((2,)), dma((2,)), dma((2 * pieces,)),
    ]
    if parts:
        H, B, _ = parts[0].shape
        outs += [jax.ShapeDtypeStruct((2 * H, B, D), BF)] * 2
        scratch += [pltpu.VMEM((len(parts), H, B, D), BF), dma((len(parts),))]
    return pl.pallas_call(
        functools.partial(_grads, work, block, pieces, S, bool(parts)),
        out_shape=outs,
        in_specs=[hbm] * len(args),
        out_specs=[hbm] * len(outs),
        scratch_shapes=scratch,
        input_output_aliases={4: 0, 5: 1} if into else {},
        compiler_params=pltpu.CompilerParams(vmem_limit_bytes=54 * 2 ** 20),
        cost_estimate=pl.CostEstimate(
            flops=2 * sum(w[3] for w in work) * T * D * block, bytes_accessed=sum(w[3] for w in work) * (2 * T * block + 4 * D * block), transcendentals=0),
        name=name,
    )(*args)


def _spread(S, parts, y, dx, sem, begin=0):
    p = lax.axis_index('stage')
    parity = lax.rem(p, 2)
    left = p < S // 2
    for k, src in enumerate(parts):
        H = src.shape[0]
        upper = parity if (begin + k) % 2 == 0 else 1 - parity
        to_dx = left if begin + k < 2 else jnp.logical_not(left)
        rows = pl.ds(upper * H, H)

        @pl.when(to_dx)
        def _():
            pltpu.make_async_copy(src, dx.at[rows], sem.at[k]).start()

        @pl.when(jnp.logical_not(to_dx))
        def _():
            pltpu.make_async_copy(src, y.at[rows], sem.at[k]).start()


def _finish(S, back, y_in, dx_in, y, dx, sem):
    _spread(S, [back], y, dx, sem, 3)
    pltpu.make_async_copy(back, y.at[pl.ds(0, back.shape[0])], sem.at[0]).wait()


def solution(mesh):
    S = mesh.shape['stage']

    def body(x, g, w1, w2):
        M, B, D = x.shape
        V, _, _, F = w1.shape
        w1 = w1[:, 0]
        w2 = w2[:, 0]
        G = GROUP
        n = V * M
        anys = pl.BlockSpec(memory_space=pl.ANY)
        dma = pltpu.SemaphoreType.DMA
        half = jax.ShapeDtypeStruct((M // 2, B, D), BF)
        u, dz, h, dy, mine, other = pl.pallas_call(
            functools.partial(_pipeline, S, V, M, G),
            out_shape=[
                jax.ShapeDtypeStruct((n, B, F), BF),
                jax.ShapeDtypeStruct((n, B, F), BF),
                jax.ShapeDtypeStruct((n, B, D), BF),
                jax.ShapeDtypeStruct((n, B, D), BF),
                half, half,
            ],
            in_specs=[anys] * 4,
            out_specs=[anys] * 6,
            scratch_shapes=[
                pltpu.VMEM((V, D, F), BF),
                pltpu.VMEM((V, F, D), BF),
                pltpu.VMEM((n, B, D), BF),
                pltpu.VMEM((n + M, B, D), BF),
                pltpu.VMEM((B, F), BF),
                pltpu.VMEM((2, B, F), BF),
                pltpu.VMEM((2, B, F), BF),
                pltpu.VMEM((2, B, D), BF),
                pltpu.VMEM((2, B, D), BF),
                dma((n,)), dma((n + M,)), dma((2,)), dma((2,)),
                dma((n,)), dma((n,)), dma((2,)), dma((2,)), dma((2 * V,)), dma((2,)), dma((M,)),
            ],
            compiler_params=pltpu.CompilerParams(
                collective_id=0, has_side_effects=True, vmem_limit_bytes=62 * 2 ** 20),
            cost_estimate=pl.CostEstimate(
                flops=10 * n * B * D * F, bytes_accessed=4 * n * B * F, transcendentals=3 * n * B * F),
            name='pipeline',
        )(x, g, w1, w2)

        h = h.reshape(V, M * B, D)
        dz = dz.reshape(V, M * B, F)
        u = u.reshape(V, M * B, F)
        dy = dy.reshape(V, M * B, D)

        far = lax.ppermute(mine, 'stage', [(q, (q + S // 2) % S) for q in range(S)])
        block = 1024 if F % 1024 == 0 else F // 3 if F % 384 == 0 else F // 2
        nb = F // block
        work = [(0, 0, 0, nb)] + [(1, v, 0, nb) for v in range(V)] + [(0, v, 0, nb) for v in range(1, V - 1)]
        d1, d2 = _grad('grads', work + [(0, V - 1, 0, nb - 2)] * (nb > 2), block, S, h, dz, u, dy)
        far, d1, d2 = lax.optimization_barrier((far, d1, d2))
        back = lax.ppermute(far, 'stage', [(q, q + 1 - 2 * (q % 2)) for q in range(S)])
        d1, d2, y, dx = _grad(
            'grads_last', [(0, V - 1, nb - 2, 2)], block, S, h, dz, u, dy, (d1, d2), (mine, other, far))
        back, d1, d2, y, dx = lax.optimization_barrier((back, d1, d2, y, dx))
        full = jax.ShapeDtypeStruct((M, B, D), BF)
        hbm = pl.BlockSpec(memory_space=pltpu.HBM)
        y, dx = pl.pallas_call(
            functools.partial(_finish, S),
            out_shape=[full, full],
            in_specs=[pl.BlockSpec(memory_space=pltpu.VMEM), hbm, hbm],
            out_specs=[hbm, hbm],
            scratch_shapes=[dma((1,))],
            input_output_aliases={1: 0, 2: 1},
            compiler_params=pltpu.CompilerParams(vmem_limit_bytes=16 * 2 ** 20),
            name='last_quarter',
        )(back, y, dx)
        return y, dx, d1[:, None], d2[:, None]

    act = P('data', None, None)
    wsp = P(None, 'stage', None, None)
    gsp = P('data', 'stage', None, None)
    return jax.shard_map(body, mesh=mesh, in_specs=(act, act, wsp, wsp), out_specs=(act, act, gsp, gsp), check_vma=False)
```

```python
import functools

import jax
import jax.numpy as jnp
from jax import lax
from jax.experimental import pallas as pl
from jax.experimental.pallas import tpu as pltpu
from jax.sharding import PartitionSpec as P

BF = jnp.bfloat16
F32 = jnp.float32
MESH = pl.DeviceIdType.MESH
NT = (((1,), (1,)), ((), ()))
GROUP = 8
ORDER = (
    'FFFFFFFFFFFFFFFFFFFFFFFBFBBBBFBFBFBFBFBFBFBFBBBBBBBBBBBBBBBBBBBB',
    'FFFFFFFFFFFFFFFFFFFBFBFBFBFBFBBFBFBFBFBFBFBFBFBBBBBBBBBBBBBBBBBB',
    'FFFFFFFFFFFBFFBFBFBFBFBFBFBFBFBFBFBFBFBFBFBFBFBFBFBFBBBBBBBBBBBB',
    'FFFFFFFFBBBFBBFBFBFBBFFFBFBFBFBFBFBFBBFBFBFBFBFBFBFBBBBBFBBBBFFF',
)
WORD = 16


def _gelu(z):
    return 0.5 * z * (1.0 + lax.erf(z * 0.7071067811865476))


def _gelu_pair(z):
    half = 0.5 * (1.0 + lax.erf(z * 0.7071067811865476))
    return z * half, half + z * jnp.exp(-0.5 * z * z) * 0.3989422804014327


def _dot(a, b):
    return jnp.dot(a, b, preferred_element_type=F32)


def _dot_nt(a, b):
    return lax.dot_general(a, b, NT, preferred_element_type=F32)


def _words(row):
    return [sum('FB'.index(c) * 2 ** b for b, c in enumerate(row[k:k + WORD])) for k in range(0, len(row), WORD)]


def _pipeline(S, V, M, G, x, g, w1_hbm, w2_hbm, u_out, dz_out, h_out, dy_out, mine, other,
              w1, w2, hbuf, dybuf, us, ub, dzb, fo, bo,
              f_recv, b_recv, f_send, b_send, h_sem, dy_sem, u_sem, dz_sem, w_sem, pair_send, pair_recv):
    p = lax.axis_index('stage')
    nxt = lax.rem(p + 1, S)
    prv = lax.rem(p + S - 1, S)
    parity = lax.rem(p, 2)
    partner = p + 1 - 2 * parity
    first = p == 0
    last = p == S - 1
    n = V * M
    H = M // 2
    F = w1.shape[-1]
    chunk = 256 if F % 256 == 0 else F

    barrier = pltpu.get_barrier_semaphore()
    for q in (prv, nxt):
        pl.semaphore_signal(barrier, inc=1, device_id={'stage': q}, device_id_type=MESH)

    def load_w(v):
        pltpu.make_async_copy(w1_hbm.at[v], w1.at[v], w_sem.at[2 * v]).start()
        pltpu.make_async_copy(w2_hbm.at[v], w2.at[v], w_sem.at[2 * v + 1]).start()

    def wait_w(v):
        pltpu.make_async_copy(w1_hbm.at[v], w1.at[v], w_sem.at[2 * v]).wait()
        pltpu.make_async_copy(w2_hbm.at[v], w2.at[v], w_sem.at[2 * v + 1]).wait()

    def load_x(m):
        pltpu.make_async_copy(x.at[m], hbuf.at[m], f_recv.at[m]).start()

    def load_g(m):
        s = (V - 1) * M + m
        pltpu.make_async_copy(g.at[m], dybuf.at[s], b_recv.at[s]).start()

    @pl.when(first)
    def _():
        load_x(0)

    load_w(0)

    @pl.when(first)
    def _():
        lax.fori_loop(1, M, lambda m, c: (load_x(m), c)[1], 0)

    for v in range(1, V):
        load_w(v)

    @pl.when(last)
    def _():
        lax.fori_loop(0, M, lambda m, c: (load_g(m), c)[1], 0)

    pl.semaphore_wait(barrier, 2)
    wait_w(0)

    def place(i):
        blk, r = i // (V * G), lax.rem(i, V * G)
        return r // G, blk * G + lax.rem(r, G)

    def place_f(i):
        v, m = place(i)
        early = i < G + G // 2
        v = jnp.where(last, jnp.where(i < G, 0, jnp.where(early, 1, jnp.where(i < 2 * G + G // 2, 0, 1))), v)
        m = jnp.where(last, jnp.where(i < G, i, jnp.where(early, i - G, jnp.where(i < 2 * G + G // 2, i - G // 2, i - 2 * G))), m)
        return v, m

    def wait_f_send(i):
        s = lax.rem(i, 2)
        pltpu.make_async_copy(fo.at[s], mine.at[0], f_send.at[s]).wait()

        @pl.when(last & (place_f(i)[0] == V - 1))
        def _():
            pltpu.make_async_copy(fo.at[s], mine.at[0], pair_send.at[s]).wait()

    def wait_b_send(j):
        s = lax.rem(j, 2)
        pltpu.make_async_copy(bo.at[s], mine.at[0], b_send.at[s]).wait()

        @pl.when(first & (place(j)[0] == V - 1))
        def _():
            pltpu.make_async_copy(bo.at[s], mine.at[0], pair_send.at[s]).wait()

    def wait_uz(s):
        pltpu.make_async_copy(ub.at[s], u_out.at[0], u_sem.at[s]).wait()
        pltpu.make_async_copy(dzb.at[s], dz_out.at[0], dz_sem.at[s]).wait()

    def take_h(slot):
        pltpu.make_async_copy(fo.at[0], hbuf.at[slot], f_recv.at[slot]).wait()
        pltpu.make_async_copy(hbuf.at[slot], h_out.at[slot], h_sem.at[slot]).start()

    def halves(m, put):
        own = m // H == parity

        @pl.when(own)
        def _():
            put(mine, other)

        @pl.when(jnp.logical_not(own))
        def _():
            put(other, mine)

    def ready_f(i):
        v, m = place_f(i)

        @pl.when(i == G - 1)
        def _():
            for vv in range(1, V):
                wait_w(vv)

        @pl.when(jnp.logical_not(last & (v == V - 1)))
        def _():
            take_h(v * M + m)

        @pl.when(i >= 2)
        def _():
            wait_f_send(i - 2)

    def compute_f(i):
        v, m = place_f(i)
        slot = v * M + m
        s = lax.rem(i, 2)
        for c in range(F // chunk):
            cs = slice(c * chunk, (c + 1) * chunk)
            us[:, cs] = _gelu(_dot(hbuf[slot], w1[v, :, cs])).astype(BF)
        fo[s] = (hbuf[slot].astype(F32) + _dot(us[...], w2[v])).astype(BF)

    def done_f(i):
        v, m = place_f(i)
        slot = v * M + m
        s = lax.rem(i, 2)
        final = last & (v == V - 1)

        @pl.when(final)
        def _():
            k = lax.rem(m, H)

            def put(here, there):
                pltpu.make_async_copy(fo.at[s], here.at[k], f_send.at[s]).start()
                pltpu.make_async_remote_copy(
                    src_ref=fo.at[s], dst_ref=there.at[k], send_sem=pair_send.at[s], recv_sem=pair_recv.at[m],
                    device_id={'stage': partner}, device_id_type=MESH).start()

            halves(m, put)

        @pl.when(jnp.logical_not(final))
        def _():
            to = slot + jnp.where(last, M, 0)
            pltpu.make_async_remote_copy(
                src_ref=fo.at[s], dst_ref=hbuf.at[to], send_sem=f_send.at[s], recv_sem=f_recv.at[to],
                device_id={'stage': nxt}, device_id_type=MESH).start()

    def place_b(j):
        vr, m = place(j)
        return V - 1 - vr, m

    def ready_b(j):
        v, m = place_b(j)
        slot = v * M + m

        @pl.when(last & (v == V - 1))
        def _():
            take_h(slot)

        pltpu.make_async_copy(bo.at[0], dybuf.at[slot], b_recv.at[slot]).wait()
        pltpu.make_async_copy(dybuf.at[slot], dy_out.at[slot], dy_sem.at[slot]).start()

        @pl.when(j >= 2)
        def _():
            wait_b_send(j - 2)
            wait_uz(lax.rem(j, 2))

    def compute_b(j):
        v, m = place_b(j)
        slot = v * M + m
        s = lax.rem(j, 2)
        for c in range(F // chunk):
            cs = slice(c * chunk, (c + 1) * chunk)
            a, b = _gelu_pair(_dot(hbuf[slot], w1[v, :, cs]))
            ub[s, :, cs] = a.astype(BF)
            dzb[s, :, cs] = (_dot_nt(dybuf[slot], w2[v, cs, :]) * b).astype(BF)
        pltpu.make_async_copy(ub.at[s], u_out.at[slot], u_sem.at[s]).start()
        bo[s] = (dybuf[slot].astype(F32) + _dot_nt(dzb[s], w1[v])).astype(BF)

    def done_b(j):
        v, m = place_b(j)
        slot = v * M + m
        s = lax.rem(j, 2)
        final = first & (v == 0)

        @pl.when(final)
        def _():
            k = lax.rem(m, H)

            def put(here, there):
                pltpu.make_async_copy(bo.at[s], here.at[k], b_send.at[s]).start()
                pltpu.make_async_remote_copy(
                    src_ref=bo.at[s], dst_ref=there.at[k], send_sem=pair_send.at[s], recv_sem=pair_recv.at[m],
                    device_id={'stage': partner}, device_id_type=MESH).start()

            halves(m, put)

        @pl.when(jnp.logical_not(final))
        def _():
            to = slot - jnp.where(first, M, 0)
            pltpu.make_async_remote_copy(
                src_ref=bo.at[s], dst_ref=dybuf.at[to], send_sem=b_send.at[s], recv_sem=b_recv.at[to],
                device_id={'stage': prv}, device_id_type=MESH).start()

        pltpu.make_async_copy(dzb.at[s], dz_out.at[slot], dz_sem.at[s]).start()

    table = [_words(row) for row in ORDER]

    def word(k):
        out = jnp.int32(0)
        for q in range(S):
            for b in range(len(table[q])):
                out = jnp.where((p == q) & (k == b), table[q][b], out)
        return out

    def step(t, carry):
        i, j, bits = carry
        bits = jnp.where(lax.rem(t, WORD) == 0, word(t // WORD), bits)
        kind = lax.rem(bits, 2)

        @pl.when(kind == 0)
        def _():
            ready_f(i)
            compute_f(i)
            done_f(i)

        @pl.when(kind == 1)
        def _():
            ready_b(j)
            compute_b(j)
            done_b(j)

        return i + 1 - kind, j + kind, bits // 2

    zero = jnp.int32(0)
    lax.fori_loop(0, 2 * n, step, (zero, zero, zero))

    for k in (n - 2, n - 1):
        wait_f_send(jnp.int32(k))
        wait_b_send(jnp.int32(k))
        wait_uz(k % 2)

    def drain(slot, carry):
        pltpu.make_async_copy(hbuf.at[slot], h_out.at[slot], h_sem.at[slot]).wait()
        pltpu.make_async_copy(dybuf.at[slot], dy_out.at[slot], dy_sem.at[slot]).wait()
        return carry

    lax.fori_loop(0, n, drain, 0)

    @pl.when(jnp.logical_not(first | last))
    def _():
        lax.fori_loop(
            0, M, lambda m, c: (pltpu.make_async_copy(fo.at[0], mine.at[0], pair_recv.at[m]).wait(), c)[1], 0)


def _grads(work, block, pieces, S, spread, h, dz, u, dy, *rest):
    if spread:
        parts = rest[2:5]
        d1, d2, y, dx, narrow, wide, o1, o2, n_sem, w_sem, o_sem, p_sem, stage, s_sem = rest[-14:]
        loads = [pltpu.make_async_copy(ref, stage.at[k], s_sem.at[k]) for k, ref in enumerate(parts)]
    else:
        d1, d2, narrow, wide, o1, o2, n_sem, w_sem, o_sem, p_sem = rest[-10:]
    T = wide.shape[1]
    begin = [sum(w[3] for w in work[:q]) for q in range(len(work) + 1)]
    total = begin[-1]
    tn = (((0,), (0,)), ((), ()))
    kinds = [w[0] for w in work]

    def pick(s, values):
        out = jnp.int32(values[0])
        for q in range(1, len(work)):
            out = jnp.where(s >= begin[q], values[q], out)
        return out

    def at(s):
        v = pick(s, [w[1] for w in work])
        blk = s + pick(s, [w[2] - begin[q] for q, w in enumerate(work)])
        return pick(s, kinds), v, pl.ds(pl.multiple_of(blk * block, block), block), lax.rem(s, 2)

    def narrow_copy(q, act):
        act(pltpu.make_async_copy((dy if kinds[q] else h).at[work[q][1]], narrow.at[q % 2], n_sem.at[q % 2]))

    def wide_copy(s, act):
        kind, v, cols, slot = at(s)
        for k, src in ((0, dz), (1, u)):
            if k in kinds:
                @pl.when(kind == k)
                def _():
                    act(pltpu.make_async_copy(src.at[v, :, cols], wide.at[slot], w_sem.at[slot]))

    def out_copy(s, act):
        kind, v, cols, slot = at(s)
        if 0 in kinds:
            @pl.when(kind == 0)
            def _():
                act(pltpu.make_async_copy(o1.at[slot], d1.at[v, :, cols], o_sem.at[slot]))
        if 1 in kinds:
            @pl.when(kind == 1)
            def _():
                act(pltpu.make_async_copy(o2.at[slot], d2.at[v, cols, :], o_sem.at[slot]))

    start = lambda c: c.start()
    wait = lambda c: c.wait()
    rows = T // pieces

    def piece(r, act):
        sl = pl.ds(pl.multiple_of(r * rows, rows), rows)
        act(pltpu.make_async_copy(h.at[work[0][1], sl], narrow.at[0, sl], p_sem.at[2 * r]))
        act(pltpu.make_async_copy(dz.at[work[0][1], sl, pl.ds(work[0][2] * block, block)], wide.at[0, sl], p_sem.at[2 * r + 1]))

    for r in range(pieces):
        piece(r, start)
    wide_copy(jnp.int32(1), start)
    if len(work) > 1:
        narrow_copy(1, start)
    if spread:
        for c in loads:
            c.start()

    piece(0, wait)
    o1[0] = lax.dot_general(narrow[0, :rows], wide[0, :rows], tn, preferred_element_type=F32)

    def add(r, carry):
        piece(r, wait)
        sl = pl.ds(pl.multiple_of(r * rows, rows), rows)
        o1[0] += lax.dot_general(narrow[0, sl], wide[0, sl], tn, preferred_element_type=F32)
        return carry

    lax.fori_loop(1, pieces, add, jnp.int32(0))
    out_copy(jnp.int32(0), start)
    if spread:
        for c in loads:
            c.wait()
        _spread(S, [stage.at[k] for k in range(len(parts))], y, dx, s_sem)

    def step(s, carry):
        kind, _, _, slot = at(s)
        side = pick(s, [q % 2 for q in range(len(work))])
        wide_copy(s, wait)
        for q in range(1, len(work)):
            @pl.when(s == begin[q])
            def _():
                narrow_copy(q, wait)
                if q + 1 < len(work):
                    narrow_copy(q + 1, start)

        @pl.when(s + 1 < total)
        def _():
            wide_copy(s + 1, start)

        @pl.when(s >= 2)
        def _():
            out_copy(s - 2, wait)

        if 0 in kinds:
            @pl.when(kind == 0)
            def _():
                o1[slot] = lax.dot_general(narrow[side], wide[slot], tn, preferred_element_type=F32)
        if 1 in kinds:
            @pl.when(kind == 1)
            def _():
                o2[slot] = lax.dot_general(wide[slot], narrow[side], tn, preferred_element_type=F32)
        out_copy(s, start)
        return carry

    lax.fori_loop(1, total, step, jnp.int32(0))
    for s in (total - 2, total - 1):
        out_copy(jnp.int32(s), wait)
    if spread:
        for k in range(len(parts)):
            pltpu.make_async_copy(stage.at[k], y.at[pl.ds(0, stage.shape[1])], s_sem.at[k]).wait()


def _grad(name, work, block, S, h, dz, u, dy, into=None, parts=None):
    V, T, D = h.shape
    F = dz.shape[-1]
    dma = pltpu.SemaphoreType.DMA
    pieces = 4
    hbm = pl.BlockSpec(memory_space=pltpu.HBM)
    kinds = [w[0] for w in work]
    args = [h, dz, u, dy] + list(into or ()) + list(parts or ())
    outs = [jax.ShapeDtypeStruct((V, D, F), F32), jax.ShapeDtypeStruct((V, F, D), F32)]
    scratch = [
        pltpu.VMEM((2 if len(work) > 1 else 1, T, D), BF),
        pltpu.VMEM((2, T, block), BF),
        pltpu.VMEM((2, D, block), F32),
        pltpu.VMEM((2, block, D) if 1 in kinds else (8, 128), F32),
        dma((2,)), dma((2,)), dma((2,)), dma((2 * pieces,)),
    ]
    if parts:
        H, B, _ = parts[0].shape
        outs += [jax.ShapeDtypeStruct((2 * H, B, D), BF)] * 2
        scratch += [pltpu.VMEM((len(parts), H, B, D), BF), dma((len(parts),))]
    return pl.pallas_call(
        functools.partial(_grads, work, block, pieces, S, bool(parts)),
        out_shape=outs,
        in_specs=[hbm] * len(args),
        out_specs=[hbm] * len(outs),
        scratch_shapes=scratch,
        input_output_aliases={4: 0, 5: 1} if into else {},
        compiler_params=pltpu.CompilerParams(vmem_limit_bytes=54 * 2 ** 20),
        cost_estimate=pl.CostEstimate(
            flops=2 * sum(w[3] for w in work) * T * D * block, bytes_accessed=sum(w[3] for w in work) * (2 * T * block + 4 * D * block), transcendentals=0),
        name=name,
    )(*args)


def _spread(S, parts, y, dx, sem, begin=0):
    p = lax.axis_index('stage')
    parity = lax.rem(p, 2)
    left = p < S // 2
    for k, src in enumerate(parts):
        H = src.shape[0]
        upper = parity if (begin + k) % 2 == 0 else 1 - parity
        to_dx = left if begin + k < 2 else jnp.logical_not(left)
        rows = pl.ds(upper * H, H)

        @pl.when(to_dx)
        def _():
            pltpu.make_async_copy(src, dx.at[rows], sem.at[k]).start()

        @pl.when(jnp.logical_not(to_dx))
        def _():
            pltpu.make_async_copy(src, y.at[rows], sem.at[k]).start()


def _finish(S, back, y_in, dx_in, y, dx, sem):
    _spread(S, [back], y, dx, sem, 3)
    pltpu.make_async_copy(back, y.at[pl.ds(0, back.shape[0])], sem.at[0]).wait()


def solution(mesh):
    S = mesh.shape['stage']

    def body(x, g, w1, w2):
        M, B, D = x.shape
        V, _, _, F = w1.shape
        w1 = w1[:, 0]
        w2 = w2[:, 0]
        G = GROUP
        n = V * M
        anys = pl.BlockSpec(memory_space=pl.ANY)
        dma = pltpu.SemaphoreType.DMA
        half = jax.ShapeDtypeStruct((M // 2, B, D), BF)
        u, dz, h, dy, mine, other = pl.pallas_call(
            functools.partial(_pipeline, S, V, M, G),
            out_shape=[
                jax.ShapeDtypeStruct((n, B, F), BF),
                jax.ShapeDtypeStruct((n, B, F), BF),
                jax.ShapeDtypeStruct((n, B, D), BF),
                jax.ShapeDtypeStruct((n, B, D), BF),
                half, half,
            ],
            in_specs=[anys] * 4,
            out_specs=[anys] * 6,
            scratch_shapes=[
                pltpu.VMEM((V, D, F), BF),
                pltpu.VMEM((V, F, D), BF),
                pltpu.VMEM((n, B, D), BF),
                pltpu.VMEM((n, B, D), BF),
                pltpu.VMEM((B, F), BF),
                pltpu.VMEM((2, B, F), BF),
                pltpu.VMEM((2, B, F), BF),
                pltpu.VMEM((2, B, D), BF),
                pltpu.VMEM((2, B, D), BF),
                dma((n,)), dma((n,)), dma((2,)), dma((2,)),
                dma((n,)), dma((n,)), dma((2,)), dma((2,)), dma((2 * V,)), dma((2,)), dma((M,)),
            ],
            compiler_params=pltpu.CompilerParams(
                collective_id=0, has_side_effects=True, vmem_limit_bytes=62 * 2 ** 20),
            cost_estimate=pl.CostEstimate(
                flops=10 * n * B * D * F, bytes_accessed=4 * n * B * F, transcendentals=3 * n * B * F),
            name='pipeline',
        )(x, g, w1, w2)

        h = h.reshape(V, M * B, D)
        dz = dz.reshape(V, M * B, F)
        u = u.reshape(V, M * B, F)
        dy = dy.reshape(V, M * B, D)

        far = lax.ppermute(mine, 'stage', [(q, (q + S // 2) % S) for q in range(S)])
        block = 1024 if F % 1024 == 0 else F // 3 if F % 384 == 0 else F // 2
        nb = F // block
        work = [(0, 0, 0, nb)] + [(1, v, 0, nb) for v in range(V)] + [(0, v, 0, nb) for v in range(1, V - 1)]
        d1, d2 = _grad('grads', work + [(0, V - 1, 0, nb - 2)] * (nb > 2), block, S, h, dz, u, dy)
        far, d1, d2 = lax.optimization_barrier((far, d1, d2))
        back = lax.ppermute(far, 'stage', [(q, q + 1 - 2 * (q % 2)) for q in range(S)])
        d1, d2, y, dx = _grad(
            'grads_last', [(0, V - 1, nb - 2, 2)], block, S, h, dz, u, dy, (d1, d2), (mine, other, far))
        back, d1, d2, y, dx = lax.optimization_barrier((back, d1, d2, y, dx))
        full = jax.ShapeDtypeStruct((M, B, D), BF)
        hbm = pl.BlockSpec(memory_space=pltpu.HBM)
        y, dx = pl.pallas_call(
            functools.partial(_finish, S),
            out_shape=[full, full],
            in_specs=[pl.BlockSpec(memory_space=pltpu.VMEM), hbm, hbm],
            out_specs=[hbm, hbm],
            scratch_shapes=[dma((1,))],
            input_output_aliases={1: 0, 2: 1},
            compiler_params=pltpu.CompilerParams(vmem_limit_bytes=16 * 2 ** 20),
            name='last_quarter',
        )(back, y, dx)
        return y, dx, d1[:, None], d2[:, None]

    act = P('data', None, None)
    wsp = P(None, 'stage', None, None)
    gsp = P('data', 'stage', None, None)
    return jax.shard_map(body, mesh=mesh, in_specs=(act, act, wsp, wsp), out_specs=(act, act, gsp, gsp), check_vma=False)
```
